8 devices in a mesh: model: 4 (over z, y, x), fsdp: 2 (over core).
Axes of the slice: x: 2, y: 2, z: 1, core: 2. Of those that a mesh axis runs over, the one named last changes fastest.
Arguments:
- tok_ids: int32 [2, 2048], P('fsdp')
- tok_labels: int32 [2, 2048], P('fsdp')
- emb_table: bfloat16 [50304, 1024], P(('model', 'fsdp'))
- w_gate: bfloat16 [1024, 4096], P('fsdp')
- w_up: bfloat16 [1024, 4096], P('fsdp')
- w_down: bfloat16 [4096, 1024], P('fsdp')
- gain_in: float32 [1024], replicated
- gain_out: float32 [1024], replicated
Outputs:
- output 1: float32 [], replicated
- output 2: float32 [50304, 1024], P(('model', 'fsdp'))
- output 3: float32 [1024, 4096], P('fsdp')
- output 4: float32 [1024, 4096], P('fsdp')
- output 5: float32 [4096, 1024], P('fsdp')
All inputs are finite; a program needn't handle non-finite values.
Results may differ from the reference program's by a relative error of at most 0.00931599.
Values are sent between devices in bfloat16 or wider.
A program may use at most 1 GiB of HBM per device.

```python
import jax
import jax.numpy as jnp
from jax import lax

V = 50304
D = 1024
F = 4096
BATCH = 2
SEQ = 2048
HEAD_BLOCK = 64
EPS = 1e-6


def draw_tokens(base_key):
    id_key, label_key = jax.random.split(base_key)
    tok_ids = jax.random.randint(id_key, (BATCH, SEQ), 0, V, dtype=jnp.int32)
    tok_ids = tok_ids.at[0, 0].set(0).at[BATCH - 1, SEQ - 1].set(V - 1)
    tok_labels = jax.random.randint(label_key, (BATCH, SEQ), 0, V, dtype=jnp.int32)
    tok_labels = tok_labels.at[0, 0].set(V - 1).at[BATCH - 1, SEQ - 1].set(0)
    return tok_ids, tok_labels


def setup_inputs(seed: int = 0) -> dict:
    rng_keys = jax.random.split(jax.random.key(seed), 7)
    tok_ids, tok_labels = draw_tokens(rng_keys[0])
    emb_table = (jax.random.normal(rng_keys[1], (V, D), jnp.float32) * D ** -0.5).astype(jnp.bfloat16)
    w_gate = (jax.random.normal(rng_keys[2], (D, F), jnp.float32) * D ** -0.5).astype(jnp.bfloat16)
    w_up = (jax.random.normal(rng_keys[3], (D, F), jnp.float32) * D ** -0.5).astype(jnp.bfloat16)
    w_down = (jax.random.normal(rng_keys[4], (F, D), jnp.float32) * (2.0 * (F * D) ** -0.5)).astype(jnp.bfloat16)
    gain_in = jax.random.uniform(rng_keys[5], (D,), jnp.float32, 0.5, 1.5)
    gain_out = jax.random.uniform(rng_keys[6], (D,), jnp.float32, 0.5, 1.5)
    return {"tok_ids": tok_ids, "tok_labels": tok_labels, "emb_table": emb_table, "w_gate": w_gate, "w_up": w_up, "w_down": w_down, "gain_in": gain_in, "gain_out": gain_out}


def rms_scale(values, gain_vec):
    mean_sq = jnp.mean(values * values, axis=-1, keepdims=True)
    return values * lax.rsqrt(mean_sq + EPS) * gain_vec


def reference(tok_ids, tok_labels, emb_table, w_gate, w_up, w_down, gain_in, gain_out):
    num_tokens = BATCH * SEQ
    flat_ids = tok_ids.reshape(num_tokens)
    flat_labels = tok_labels.reshape(num_tokens)
    x_emb = emb_table[flat_ids].astype(jnp.float32)
    normed_in, norm_in_back = jax.vjp(lambda values: rms_scale(values, gain_in), x_emb)
    normed_bf = normed_in.astype(jnp.bfloat16)
    gate_f = jnp.dot(normed_bf, w_gate, preferred_element_type=jnp.float32).astype(jnp.bfloat16).astype(jnp.float32)
    up_f = jnp.dot(normed_bf, w_up, preferred_element_type=jnp.float32).astype(jnp.bfloat16).astype(jnp.float32)
    gate_sig = jax.nn.sigmoid(gate_f)
    silu_gate = gate_f * gate_sig
    act_bf = (silu_gate * up_f).astype(jnp.bfloat16)
    mlp_out = jnp.dot(act_bf, w_down, preferred_element_type=jnp.float32).astype(jnp.bfloat16)
    h_res = x_emb + mlp_out.astype(jnp.float32)
    hn_f, norm_out_back = jax.vjp(lambda values: rms_scale(values, gain_out), h_res)
    hn_bf = hn_f.astype(jnp.bfloat16)
    num_blocks = num_tokens // HEAD_BLOCK
    hn_blocks = hn_bf.reshape(num_blocks, HEAD_BLOCK, D)
    label_blocks = flat_labels.reshape(num_blocks, HEAD_BLOCK)

    def head_step(d_head, block_in):
        hn_blk, label_blk = block_in
        logits = jnp.dot(hn_blk, emb_table.T, preferred_element_type=jnp.float32)
        row_max = jnp.max(logits, axis=-1, keepdims=True)
        exp_shift = jnp.exp(logits - row_max)
        sum_exp = jnp.sum(exp_shift, axis=-1, keepdims=True)
        onehot = lax.broadcasted_iota(jnp.int32, logits.shape, 1) == label_blk[:, None]
        label_logit = jnp.sum(jnp.where(onehot, logits, 0.0), axis=-1)
        tok_loss = row_max[:, 0] + jnp.log(sum_exp[:, 0]) - label_logit
        soft_probs = exp_shift / sum_exp
        d_logits = (jnp.where(onehot, soft_probs - 1.0, soft_probs) / num_tokens).astype(jnp.bfloat16)
        d_head = d_head + jnp.dot(d_logits.T, hn_blk, preferred_element_type=jnp.float32)
        d_hn = jnp.dot(d_logits, emb_table, preferred_element_type=jnp.float32)
        return d_head, (tok_loss, d_hn)

    d_head, (tok_losses, d_hn_blocks) = lax.scan(head_step, jnp.zeros((V, D), jnp.float32), (hn_blocks, label_blocks))
    loss = jnp.sum(tok_losses) / num_tokens
    d_hn = d_hn_blocks.reshape(num_tokens, D)
    d_hidden = norm_out_back(d_hn)[0]
    d_mlp = d_hidden.astype(jnp.bfloat16)
    d_act = jnp.dot(d_mlp, w_down.T, preferred_element_type=jnp.float32)
    grad_down = jnp.dot(act_bf.T, d_mlp, preferred_element_type=jnp.float32)
    d_gate = (d_act * up_f * (gate_sig * (1.0 + gate_f * (1.0 - gate_sig)))).astype(jnp.bfloat16)
    d_up = (d_act * silu_gate).astype(jnp.bfloat16)
    grad_gate = jnp.dot(normed_bf.T, d_gate, preferred_element_type=jnp.float32)
    grad_up = jnp.dot(normed_bf.T, d_up, preferred_element_type=jnp.float32)
    d_normed = jnp.dot(d_gate, w_gate.T, preferred_element_type=jnp.float32) + jnp.dot(d_up, w_up.T, preferred_element_type=jnp.float32)
    d_x = d_hidden + norm_in_back(d_normed)[0]
    d_in = jax.ops.segment_sum(d_x, flat_ids, num_segments=V)
    grad_table = d_head + d_in
    return (loss, grad_table, grad_gate, grad_up, grad_down)
```

```python
import functools

import jax
import jax.numpy as jnp
from jax import lax
from jax.experimental import pallas as pl
from jax.experimental.pallas import tpu as pltpu
from jax.sharding import PartitionSpec as P

EPS = 1e-6
VMEM_LIMIT = 63 * 1024 * 1024
LANES = 128


def rms_scale(values, gain_vec):
    mean_sq = jnp.mean(values * values, axis=-1, keepdims=True)
    return values * lax.rsqrt(mean_sq + EPS) * gain_vec


def mlp_forward(x_emb, gain_in, w_gate, w_up, w_down):
    normed_in, norm_in_back = jax.vjp(lambda values: rms_scale(values, gain_in), x_emb)
    normed_bf = normed_in.astype(jnp.bfloat16)
    gate_f = jnp.dot(normed_bf, w_gate, preferred_element_type=jnp.float32).astype(jnp.bfloat16).astype(jnp.float32)
    up_f = jnp.dot(normed_bf, w_up, preferred_element_type=jnp.float32).astype(jnp.bfloat16).astype(jnp.float32)
    gate_sig = jax.nn.sigmoid(gate_f)
    silu_gate = gate_f * gate_sig
    act_bf = (silu_gate * up_f).astype(jnp.bfloat16)
    mlp_out = jnp.dot(act_bf, w_down, preferred_element_type=jnp.float32).astype(jnp.bfloat16)
    h_res = x_emb + mlp_out.astype(jnp.float32)
    return h_res, (norm_in_back, normed_bf, gate_f, up_f, gate_sig, silu_gate, act_bf)


def mlp_backward(d_hidden, saved, w_gate, w_up, w_down):
    norm_in_back, normed_bf, gate_f, up_f, gate_sig, silu_gate, act_bf = saved
    d_mlp = d_hidden.astype(jnp.bfloat16)
    d_act = jnp.einsum("td,fd->tf", d_mlp, w_down, preferred_element_type=jnp.float32)
    grad_down = jnp.einsum("tf,td->fd", act_bf, d_mlp, preferred_element_type=jnp.float32)
    d_gate = (d_act * up_f * (gate_sig * (1.0 + gate_f * (1.0 - gate_sig)))).astype(jnp.bfloat16)
    d_up = (d_act * silu_gate).astype(jnp.bfloat16)
    grad_gate = jnp.einsum("td,tf->df", normed_bf, d_gate, preferred_element_type=jnp.float32)
    grad_up = jnp.einsum("td,tf->df", normed_bf, d_up, preferred_element_type=jnp.float32)
    d_normed = jnp.einsum("tf,df->td", d_gate, w_gate, preferred_element_type=jnp.float32) + jnp.einsum("tf,df->td", d_up, w_up, preferred_element_type=jnp.float32)
    d_x = d_hidden + norm_in_back(d_normed)[0]
    return d_x, grad_gate, grad_up, grad_down


def slow_step(tok_ids, tok_labels, table_shard, gate_shard, up_shard, down_shard, gain_in, gain_out):
    fsdp_size = lax.axis_size("fsdp")
    local_count = tok_ids.shape[0] * tok_ids.shape[1]
    num_tokens = local_count * fsdp_size
    table_part = lax.all_gather(table_shard, "fsdp", axis=0, tiled=True)
    w_gate = lax.all_gather(gate_shard, "fsdp", axis=0, tiled=True)
    w_up = lax.all_gather(up_shard, "fsdp", axis=0, tiled=True)
    w_down = lax.all_gather(down_shard, "fsdp", axis=0, tiled=True)
    vocab_part = table_part.shape[0]
    vocab_start = lax.axis_index("model") * vocab_part
    local_ids = tok_ids.reshape(local_count) - vocab_start
    id_inside = (local_ids >= 0) & (local_ids < vocab_part)
    safe_ids = jnp.where(id_inside, local_ids, 0)
    emb_rows = jnp.where(id_inside[:, None], jnp.take(table_part, safe_ids, axis=0), 0)
    x_emb = lax.psum(emb_rows, "model").astype(jnp.float32)
    h_res, saved = mlp_forward(x_emb, gain_in, w_gate, w_up, w_down)
    hn_f, norm_out_back = jax.vjp(lambda values: rms_scale(values, gain_out), h_res)
    hn_bf = hn_f.astype(jnp.bfloat16)
    logits = jnp.einsum("td,vd->tv", hn_bf, table_part, preferred_element_type=jnp.float32)
    row_max = lax.pmax(jnp.max(logits, axis=-1), "model")
    exp_shift = jnp.exp(logits - row_max[:, None])
    local_labels = tok_labels.reshape(local_count) - vocab_start
    onehot = lax.broadcasted_iota(jnp.int32, logits.shape, 1) == local_labels[:, None]
    part_stats = jnp.stack([jnp.sum(exp_shift, axis=-1), jnp.sum(jnp.where(onehot, logits, 0.0), axis=-1)])
    tok_stats = lax.psum(part_stats, "model")
    sum_exp = tok_stats[0]
    tok_loss = row_max + jnp.log(sum_exp) - tok_stats[1]
    loss = lax.psum(jnp.sum(tok_loss), "fsdp") / num_tokens
    soft_probs = exp_shift / sum_exp[:, None]
    d_logits = (jnp.where(onehot, soft_probs - 1.0, soft_probs) / num_tokens).astype(jnp.bfloat16)
    d_head = jnp.einsum("tv,td->vd", d_logits, hn_bf, preferred_element_type=jnp.float32)
    d_hn = lax.psum(jnp.einsum("tv,vd->td", d_logits, table_part, preferred_element_type=jnp.float32), "model")
    d_hidden = norm_out_back(d_hn)[0]
    d_x, grad_gate, grad_up, grad_down = mlp_backward(d_hidden, saved, w_gate, w_up, w_down)
    d_in = jax.ops.segment_sum(jnp.where(id_inside[:, None], d_x, 0.0), safe_ids, num_segments=vocab_part)
    grad_table = lax.psum_scatter(d_head + d_in, "fsdp", scatter_dimension=0, tiled=True)
    grad_gate = lax.psum_scatter(grad_gate, "fsdp", scatter_dimension=0, tiled=True)
    grad_up = lax.psum_scatter(grad_up, "fsdp", scatter_dimension=0, tiled=True)
    grad_down = lax.psum_scatter(grad_down, "fsdp", scatter_dimension=0, tiled=True)
    return loss, grad_table, grad_gate, grad_up, grad_down


def lane_chunks(width, chunk):
    return [(lo, min(chunk, width - lo)) for lo in range(0, width, chunk)]

def logits_kernel(chunk, hn_ref, emb_ref, lab_ref, z_ref, stat_ref):
    rows, vocab = z_ref.shape
    hn = hn_ref[...]
    label = lab_ref[...]
    lane = lax.broadcasted_iota(jnp.int32, (rows, LANES), 1)
    run_max = jnp.full((rows, LANES), -jnp.inf, jnp.float32)
    run_sum = jnp.zeros((rows, LANES), jnp.float32)
    run_lab = jnp.zeros((rows, LANES), jnp.float32)
    tail = None
    for lo, width in lane_chunks(vocab, chunk):
        z = lax.dot_general(hn, emb_ref[lo:lo + width, :], (((1,), (1,)), ((), ())), preferred_element_type=jnp.float32)
        z_ref[:, lo:lo + width] = z
        groups = width // LANES
        new_max = run_max
        for g in range(groups):
            part = z[:, g * LANES:(g + 1) * LANES]
            new_max = jnp.maximum(new_max, part)
            run_lab = run_lab + jnp.where(lane == label - (lo + g * LANES), part, 0.0)
        run_sum = run_sum * jnp.exp(run_max - new_max)
        for g in range(groups):
            run_sum = run_sum + jnp.exp(z[:, g * LANES:(g + 1) * LANES] - new_max)
        run_max = new_max
        if width % LANES:
            tail = (lo + groups * LANES, z[:, groups * LANES:])
    row_max = jnp.max(run_max, axis=1, keepdims=True)
    if tail is not None:
        row_max = jnp.maximum(row_max, jnp.max(tail[1], axis=1, keepdims=True))
    row_sum = jnp.sum(run_sum * jnp.exp(run_max - row_max), axis=1, keepdims=True)
    row_lab = jnp.sum(run_lab, axis=1, keepdims=True)
    if tail is not None:
        start, z = tail
        tail_lane = lax.broadcasted_iota(jnp.int32, z.shape, 1)
        row_sum = row_sum + jnp.sum(jnp.exp(z - row_max), axis=1, keepdims=True)
        row_lab = row_lab + jnp.sum(jnp.where(tail_lane == label - start, z, 0.0), axis=1, keepdims=True)
    stat_ref[...] = jnp.where(lane == 0, row_max, jnp.where(lane == 1, row_sum, row_lab))

def head_logits(hn, table, labels, blk=256, chunk=1024):
    tokens, depth = hn.shape
    vocab = table.shape[0]
    return pl.pallas_call(
        functools.partial(logits_kernel, chunk),
        grid=(tokens // blk,),
        in_specs=[
            pl.BlockSpec((blk, depth), lambda i: (i, 0)),
            pl.BlockSpec((vocab, depth), lambda i: (0, 0), pipeline_mode=pl.Buffered(1)),
            pl.BlockSpec((blk, 1), lambda i: (i, 0)),
        ],
        out_specs=[
            pl.BlockSpec((blk, vocab), lambda i: (i, 0)),
            pl.BlockSpec((blk, LANES), lambda i: (i, 0)),
        ],
        out_shape=[jax.ShapeDtypeStruct((tokens, vocab), jnp.float32), jax.ShapeDtypeStruct((tokens, LANES), jnp.float32)],
        cost_estimate=pl.CostEstimate(flops=2 * tokens * vocab * depth, bytes_accessed=4 * tokens * vocab, transcendentals=tokens * vocab),
        compiler_params=pltpu.CompilerParams(vmem_limit_bytes=VMEM_LIMIT),
        name="head_logits",
    )(hn, table, labels)

def dlogits_kernel(inv_tokens, chunk, z_ref, emb_ref, stat_ref, lab_ref, dz_ref, dhn_ref):
    rows, vocab = z_ref.shape
    row_max = stat_ref[:, 0:1]
    scale = stat_ref[:, 1:2]
    label = lab_ref[...]
    total = None
    for n, (lo, width) in enumerate(lane_chunks(vocab, chunk)):
        prob = jnp.exp(z_ref[:, lo:lo + width] - row_max) * scale
        lane = lax.broadcasted_iota(jnp.int32, (rows, width), 1)
        prob = jnp.where(lane == label - lo, prob - 1.0, prob)
        dz = (prob * inv_tokens).astype(jnp.bfloat16)
        dz_ref[:, lo:lo + width] = dz
        part = jnp.dot(dz, emb_ref[lo:lo + width, :], preferred_element_type=jnp.float32)
        total = part if total is None else total + part
    dhn_ref[...] = total

def head_dlogits(z, table, stats, labels, inv_tokens, blk=256, chunk=1024):
    tokens, vocab = z.shape
    depth = table.shape[1]
    return pl.pallas_call(
        functools.partial(dlogits_kernel, inv_tokens, chunk),
        grid=(tokens // blk,),
        in_specs=[
            pl.BlockSpec((blk, vocab), lambda i: (i, 0)),
            pl.BlockSpec((vocab, depth), lambda i: (0, 0), pipeline_mode=pl.Buffered(1)),
            pl.BlockSpec((blk, LANES), lambda i: (i, 0)),
            pl.BlockSpec((blk, 1), lambda i: (i, 0)),
        ],
        out_specs=[
            pl.BlockSpec((blk, vocab), lambda i: (i, 0)),
            pl.BlockSpec((blk, depth), lambda i: (i, 0)),
        ],
        out_shape=[jax.ShapeDtypeStruct((tokens, vocab), jnp.bfloat16), jax.ShapeDtypeStruct((tokens, depth), jnp.float32)],
        cost_estimate=pl.CostEstimate(flops=2 * tokens * vocab * depth, bytes_accessed=6 * tokens * vocab, transcendentals=tokens * vocab),
        compiler_params=pltpu.CompilerParams(vmem_limit_bytes=VMEM_LIMIT),
        name="head_dlogits",
    )(z, table, stats, labels)

TN = (((0,), (0,)), ((), ()))
NT = (((1,), (1,)), ((), ()))

def dhead_kernel(a_ref, ha_ref, b_ref, hb_ref, out_ref):
    out_ref[...] = (lax.dot_general(a_ref[...], ha_ref[...], TN, preferred_element_type=jnp.float32)
                    + lax.dot_general(b_ref[...], hb_ref[...], TN, preferred_element_type=jnp.float32))

def head_dtable(dz_a, hn_a, dz_b, hn_b, tile=640):
    tokens, vocab = dz_a.shape
    depth = hn_a.shape[1]
    dz_spec = pl.BlockSpec((tokens, tile), lambda i: (0, i))
    hn_spec = pl.BlockSpec((tokens, depth), lambda i: (0, 0), pipeline_mode=pl.Buffered(1))
    return pl.pallas_call(
        dhead_kernel,
        grid=(pl.cdiv(vocab, tile),),
        in_specs=[dz_spec, hn_spec, dz_spec, hn_spec],
        out_specs=pl.BlockSpec((tile, depth), lambda i: (i, 0)),
        out_shape=jax.ShapeDtypeStruct((vocab, depth), jnp.float32),
        cost_estimate=pl.CostEstimate(flops=4 * tokens * vocab * depth, bytes_accessed=4 * tokens * vocab + 4 * vocab * depth, transcendentals=0),
        compiler_params=pltpu.CompilerParams(vmem_limit_bytes=VMEM_LIMIT),
        name="head_dtable",
    )(dz_a, hn_a, dz_b, hn_b)

def norm(values, gain):
    return values * lax.rsqrt(jnp.mean(values * values, axis=-1, keepdims=True) + EPS) * gain

def mlp_kernel(chunk, x_ref, g1_ref, g2_ref, wg_ref, wu_ref, wd_ref, a_ref, gt_ref, up_ref, q_ref, h_ref, hn_ref):
    x = x_ref[...]
    a = norm(x, g1_ref[...]).astype(jnp.bfloat16)
    a_ref[...] = a
    total = None
    for lo in range(0, gt_ref.shape[1], chunk):
        cols = slice(lo, lo + chunk)
        gt = jnp.dot(a, wg_ref[:, cols], preferred_element_type=jnp.float32).astype(jnp.bfloat16)
        up = jnp.dot(a, wu_ref[:, cols], preferred_element_type=jnp.float32).astype(jnp.bfloat16)
        gt_ref[:, cols] = gt
        up_ref[:, cols] = up
        gate = gt.astype(jnp.float32)
        q = (gate * jax.nn.sigmoid(gate) * up.astype(jnp.float32)).astype(jnp.bfloat16)
        q_ref[:, cols] = q
        part = jnp.dot(q, wd_ref[cols, :], preferred_element_type=jnp.float32)
        total = part if total is None else total + part
    h = x + total.astype(jnp.bfloat16).astype(jnp.float32)
    h_ref[...] = h
    hn_ref[...] = norm(h, g2_ref[...]).astype(jnp.bfloat16)

def mlp_forward_kernel(x, g1, g2, wg, wu, wd, tokens, blk=256, chunk=1024):
    depth = x.shape[1]
    width = wg.shape[1]
    row = lambda n: pl.BlockSpec((blk, n), lambda i: (i, 0))
    whole = lambda s: pl.BlockSpec(s, lambda i: (0, 0), pipeline_mode=pl.Buffered(1))
    shape = lambda n, t: jax.ShapeDtypeStruct((tokens, n), t)
    return pl.pallas_call(
        functools.partial(mlp_kernel, chunk),
        grid=(tokens // blk,),
        in_specs=[row(depth), whole((1, depth)), whole((1, depth)), whole(wg.shape), whole(wu.shape), whole(wd.shape)],
        out_specs=[row(depth), row(width), row(width), row(width), row(depth), row(depth)],
        out_shape=[shape(depth, jnp.bfloat16), shape(width, jnp.bfloat16), shape(width, jnp.bfloat16), shape(width, jnp.bfloat16), shape(depth, jnp.float32), shape(depth, jnp.bfloat16)],
        cost_estimate=pl.CostEstimate(flops=6 * tokens * width * depth, bytes_accessed=6 * tokens * width, transcendentals=tokens * width),
        compiler_params=pltpu.CompilerParams(vmem_limit_bytes=VMEM_LIMIT),
        name="mlp_forward",
    )(x, g1.reshape(1, -1), g2.reshape(1, -1), wg, wu, wd)

def dact_kernel(chunk, dm_ref, wd_ref, gt_ref, up_ref, dgt_ref, dup_ref):
    dm = dm_ref[...]
    for lo in range(0, gt_ref.shape[1], chunk):
        cols = slice(lo, lo + chunk)
        dq = lax.dot_general(dm, wd_ref[cols, :], NT, preferred_element_type=jnp.float32)
        gate = gt_ref[:, cols].astype(jnp.float32)
        up = up_ref[:, cols].astype(jnp.float32)
        sig = jax.nn.sigmoid(gate)
        dgt_ref[:, cols] = (dq * up * (sig * (1.0 + gate * (1.0 - sig)))).astype(jnp.bfloat16)
        dup_ref[:, cols] = (dq * (gate * sig)).astype(jnp.bfloat16)

def mlp_dact(dm, wd, gt, up, blk=256, chunk=1024):
    tokens, depth = dm.shape
    width = wd.shape[0]
    row = lambda n: pl.BlockSpec((blk, n), lambda i: (i, 0))
    return pl.pallas_call(
        functools.partial(dact_kernel, chunk),
        grid=(tokens // blk,),
        in_specs=[row(depth), pl.BlockSpec(wd.shape, lambda i: (0, 0), pipeline_mode=pl.Buffered(1)), row(width), row(width)],
        out_specs=[row(width), row(width)],
        out_shape=[jax.ShapeDtypeStruct((tokens, width), jnp.bfloat16)] * 2,
        cost_estimate=pl.CostEstimate(flops=2 * tokens * width * depth, bytes_accessed=8 * tokens * width, transcendentals=tokens * width),
        compiler_params=pltpu.CompilerParams(vmem_limit_bytes=VMEM_LIMIT),
        name="mlp_dact",
    )(dm, wd, gt, up)

def dweight_kernel(a_ref, b_ref, out_ref):
    out_ref[...] = lax.dot_general(a_ref[...], b_ref[...], TN, preferred_element_type=jnp.float32)

def dweight(a, b, rows, cols):
    tokens, m = a.shape
    n = b.shape[1]
    whole = pl.Buffered(1)
    a_spec = pl.BlockSpec((tokens, rows), lambda i, j: (0, i)) if rows < m else pl.BlockSpec((tokens, m), lambda i, j: (0, 0), pipeline_mode=whole)
    b_spec = pl.BlockSpec((tokens, cols), lambda i, j: (0, j)) if cols < n else pl.BlockSpec((tokens, n), lambda i, j: (0, 0), pipeline_mode=whole)
    return pl.pallas_call(
        dweight_kernel,
        grid=(m // rows, n // cols),
        in_specs=[a_spec, b_spec],
        out_specs=pl.BlockSpec((rows, cols), lambda i, j: (i, j)),
        out_shape=jax.ShapeDtypeStruct((m, n), jnp.float32),
        cost_estimate=pl.CostEstimate(flops=2 * tokens * m * n, bytes_accessed=2 * tokens * (m + n) + 4 * m * n, transcendentals=0),
        compiler_params=pltpu.CompilerParams(vmem_limit_bytes=VMEM_LIMIT),
        name="dweight",
    )(a, b)


def add_rows_kernel(bound_ref, ids_ref, base_ref, rows_ref, out_ref):
    tile = pl.program_id(0)
    out_ref[...] = base_ref[...]
    start = tile * out_ref.shape[0]
    for part in range(rows_ref.shape[0]):
        def body(t, carry, part=part):
            row = ids_ref[part, t] - start
            out_ref[pl.ds(row, 1), :] = out_ref[pl.ds(row, 1), :] + rows_ref[part, pl.ds(t, 1), :]
            return carry
        lax.fori_loop(bound_ref[part, tile], bound_ref[part, tile + 1], body, 0)


def add_rows(base, rows, ids, bounds, tile):
    vocab, depth = base.shape
    return pl.pallas_call(
        add_rows_kernel,
        grid_spec=pltpu.PrefetchScalarGridSpec(
            num_scalar_prefetch=2,
            grid=(vocab // tile,),
            in_specs=[
                pl.BlockSpec((tile, depth), lambda i, *_: (i, 0)),
                pl.BlockSpec(rows.shape, lambda i, *_: (0, 0, 0), pipeline_mode=pl.Buffered(1)),
            ],
            out_specs=pl.BlockSpec((tile, depth), lambda i, *_: (i, 0)),
        ),
        out_shape=jax.ShapeDtypeStruct(base.shape, base.dtype),
        input_output_aliases={2: 0},
        cost_estimate=pl.CostEstimate(flops=2 * vocab * depth, bytes_accessed=8 * vocab * depth, transcendentals=0),
        compiler_params=pltpu.CompilerParams(vmem_limit_bytes=VMEM_LIMIT),
        name="add_rows",
    )(bounds, ids, base, rows)


def place_kernel(start_ref, blocks_ref, out_ref, *scratch):
    rows = scratch[0] if scratch else out_ref
    blocks, cap, depth = blocks_ref.shape
    sub = lax.broadcasted_iota(jnp.int32, (8, depth), 0)
    for b in range(blocks):
        base = pl.multiple_of(start_ref[b] // 8 * 8, 8)
        shift = start_ref[b] % 8
        turned = pltpu.roll(blocks_ref[b].astype(jnp.float32), shift, 0)
        head = turned[:8]
        rows[pl.ds(base, 8), :] = jnp.where(sub < shift, rows[pl.ds(base, 8), :], head)
        rows[pl.ds(pl.multiple_of(base + 8, 8), cap - 8), :] = turned[8:]
        tail = pl.ds(pl.multiple_of(base + cap, 8), 8)
        rows[tail, :] = jnp.where(sub < shift, head, rows[tail, :])
    if scratch:
        out_ref[...] = rows[:out_ref.shape[0]].astype(out_ref.dtype)


def place_rows(blocks, starts, count, dtype):
    depth = blocks.shape[2]
    in_vmem = pl.BlockSpec(memory_space=pltpu.VMEM)
    return pl.pallas_call(
        place_kernel,
        in_specs=[pl.BlockSpec(memory_space=pltpu.SMEM), in_vmem],
        out_specs=in_vmem,
        out_shape=jax.ShapeDtypeStruct((count, depth), dtype),
        scratch_shapes=[] if dtype == jnp.float32 else [pltpu.VMEM((count + 8, depth), jnp.float32)],
        cost_estimate=pl.CostEstimate(flops=8 * count * depth, bytes_accessed=8 * count * depth, transcendentals=0),
        compiler_params=pltpu.CompilerParams(vmem_limit_bytes=VMEM_LIMIT),
        name="place_rows",
    )(starts, blocks)


def window_kernel(first_ref, a_ref, b_ref, out_ref, total_ref):
    count, depth = a_ref.shape
    windows, cap, _ = out_ref.shape
    total_ref[:count] = a_ref[...] + b_ref[...]
    for c in range(windows):
        base = pl.multiple_of(first_ref[c] // 8 * 8, 8)
        shift = first_ref[c] % 8
        piece = total_ref[pl.ds(base, cap + 8), :]
        out_ref[c] = pltpu.roll(piece, (cap + 8) - shift, 0)[:cap]


def sum_windows(a, b, first, cap):
    depth = a.shape[1]
    in_vmem = pl.BlockSpec(memory_space=pltpu.VMEM)
    return pl.pallas_call(
        window_kernel,
        in_specs=[pl.BlockSpec(memory_space=pltpu.SMEM), in_vmem, in_vmem],
        out_specs=in_vmem,
        out_shape=jax.ShapeDtypeStruct((first.shape[0], cap, depth), jnp.float32),
        scratch_shapes=[pltpu.VMEM((a.shape[0] + 8, depth), jnp.float32)],
        cost_estimate=pl.CostEstimate(flops=8 * a.size, bytes_accessed=12 * a.size, transcendentals=0),
        compiler_params=pltpu.CompilerParams(vmem_limit_bytes=VMEM_LIMIT),
        name="sum_windows",
    )(first, a, b)


def swap_cores(values):
    return lax.ppermute(values, "fsdp", [(0, 1), (1, 0)])


def fast_step(sorted_ids, sorted_labels, starts, sizes, table_shard, gate_shard, up_shard, down_shard, gain_in, gain_out):
    model_size, fsdp_size, dev_cap, chip_cap = sizes
    vocab, depth = table_shard.shape
    chip = lax.axis_index("model")
    core = lax.axis_index("fsdp")
    device = chip * fsdp_size + core
    count = sorted_ids.shape[1]
    num_tokens = count * fsdp_size
    own = lambda values: lax.dynamic_index_in_dim(values, core, 0, keepdims=False)
    other = lambda values: lax.dynamic_index_in_dim(values, 1 - core, 0, keepdims=False)

    w_gate = lax.all_gather(gate_shard, "fsdp", axis=0, tiled=True)
    w_up = lax.all_gather(up_shard, "fsdp", axis=0, tiled=True)
    with jax.named_scope("gather_rows"):
        slot = lax.dynamic_slice(starts, (0, device), (fsdp_size, 1)) + jnp.arange(dev_cap, dtype=jnp.int32)[None, :]
        wanted = jnp.take_along_axis(sorted_ids, jnp.minimum(slot, count - 1), axis=1) - device * vocab
        rows = jnp.take(table_shard, jnp.clip(wanted, 0, vocab - 1).reshape(-1), axis=0, mode="clip").reshape(fsdp_size, dev_cap, depth)
        theirs = swap_cores(other(rows))
        mine = own(rows)
        pair = jnp.where(core == 0, jnp.stack([mine, theirs]), jnp.stack([theirs, mine]))
        pair, w_gate, w_up = lax.optimization_barrier((pair, w_gate, w_up))
        blocks = lax.all_gather(pair, "model", axis=0, tiled=True)
        my_starts = own(starts)
        x_buf = place_rows(blocks, my_starts, count + dev_cap + 8, jnp.float32)
    w_down = lax.all_gather(down_shard, "fsdp", axis=0, tiled=True)

    normed_bf, gate_bf, up_bf, act_bf, h_res, hn_own = mlp_forward_kernel(x_buf, gain_in, gain_out, w_gate, w_up, w_down, count)
    hn_other = swap_cores(hn_own)
    local_labels = sorted_labels - device * vocab
    labels_own = own(local_labels)[:, None]
    labels_other = other(local_labels)[:, None]
    z_own, stat_own = head_logits(hn_own, table_shard, labels_own)
    z_other, stat_other = head_logits(hn_other, table_shard, labels_other)
    part_own = stat_own[:, :3].T
    part_other = stat_other[:, :3].T
    part = jnp.where(core == 0, jnp.stack([part_own, part_other]), jnp.stack([part_other, part_own]))
    all_stats = lax.all_gather(part.reshape(fsdp_size * 3, count), ("model", "fsdp"), axis=0).reshape(-1, fsdp_size, 3, count)
    row_max = jnp.max(all_stats[:, :, 0], axis=0)
    sum_exp = jnp.sum(all_stats[:, :, 1] * jnp.exp(all_stats[:, :, 0] - row_max[None]), axis=0)
    label_logit = jnp.sum(all_stats[:, :, 2], axis=0)
    loss = jnp.sum(row_max + jnp.log(sum_exp) - label_logit) / num_tokens
    lane = lax.broadcasted_iota(jnp.int32, (fsdp_size, count, LANES), 2)
    stats = jnp.where(lane == 0, row_max[:, :, None], (1.0 / sum_exp)[:, :, None])
    dz_other, d_hn_other = head_dlogits(z_other, table_shard, other(stats), labels_other, 1.0 / num_tokens)
    d_hn_theirs = swap_cores(d_hn_other)
    dz_own, d_hn_own = head_dlogits(z_own, table_shard, own(stats), labels_own, 1.0 / num_tokens)

    first = jnp.minimum(my_starts[0:model_size * fsdp_size:fsdp_size], count - chip_cap)
    windows = sum_windows(d_hn_own, d_hn_theirs, first, chip_cap)
    d_hn = lax.psum_scatter(windows.reshape(model_size * chip_cap, depth), "model", scatter_dimension=0, tiled=True)
    d_head = head_dtable(dz_own, hn_own, dz_other, hn_other)
    d_hn, d_head = lax.optimization_barrier((d_hn, d_head))
    my_first = lax.dynamic_index_in_dim(first, chip, 0, keepdims=False)
    h_window = lax.dynamic_slice(h_res, (my_first, 0), (chip_cap, depth))
    _, norm_out_back = jax.vjp(lambda values: rms_scale(values, gain_out), h_window)
    d_hidden = norm_out_back(d_hn)[0]
    dm_blocks = lax.all_gather(d_hidden.astype(jnp.bfloat16), "model", axis=0)
    d_mlp = place_rows(dm_blocks, first, count, jnp.bfloat16)

    d_gate, d_up = mlp_dact(d_mlp, w_down, gate_bf, up_bf)
    grad_down = jnp.einsum("tf,td->fd", act_bf, d_mlp, preferred_element_type=jnp.float32)
    grad_gate = jnp.einsum("td,tf->df", normed_bf, d_gate, preferred_element_type=jnp.float32)
    grad_up = jnp.einsum("td,tf->df", normed_bf, d_up, preferred_element_type=jnp.float32)
    d_gate_own = lax.dynamic_slice(d_gate, (my_first, 0), (chip_cap, d_gate.shape[1]))
    d_up_own = lax.dynamic_slice(d_up, (my_first, 0), (chip_cap, d_up.shape[1]))
    x_window = lax.dynamic_slice(x_buf, (my_first, 0), (chip_cap, depth))
    d_normed = jnp.einsum("tf,df->td", d_gate_own, w_gate, preferred_element_type=jnp.float32) + jnp.einsum("tf,df->td", d_up_own, w_up, preferred_element_type=jnp.float32)
    _, norm_in_back = jax.vjp(lambda values: rms_scale(values, gain_in), x_window)
    d_x = d_hidden + norm_in_back(d_normed)[0]
    d_x_theirs = swap_cores(d_x)
    d_x_pair = jnp.where(core == 0, jnp.stack([d_x, d_x_theirs]), jnp.stack([d_x_theirs, d_x]))

    tile = vocab // 6
    pair_first = jnp.minimum(lax.dynamic_index_in_dim(starts, chip * fsdp_size, 1, keepdims=False), count - chip_cap)
    own_ids = jnp.stack([lax.dynamic_slice(sorted_ids[p], (pair_first[p],), (chip_cap,)) for p in range(fsdp_size)]) - device * vocab
    edges = jnp.arange(vocab // tile + 1, dtype=jnp.int32) * tile
    bounds = jnp.sum((own_ids[:, :, None] < edges[None, None, :]).astype(jnp.int32), axis=1)
    grad_table = add_rows(d_head, d_x_pair, own_ids, bounds, tile)

    grad_gate = lax.psum_scatter(grad_gate, "fsdp", scatter_dimension=0, tiled=True)
    grad_up = lax.psum_scatter(grad_up, "fsdp", scatter_dimension=0, tiled=True)
    grad_down = lax.psum_scatter(grad_down, "fsdp", scatter_dimension=0, tiled=True)
    return loss, grad_table, grad_gate, grad_up, grad_down


def capacity(tokens, shares, lists):
    mean = tokens / shares
    return -(-int((mean + 4.5 * mean ** 0.5) / lists) // 16) * 16


def solution(mesh):
    fsdp_size = mesh.shape["fsdp"]
    model_size = mesh.shape["model"]
    tok_spec = P("fsdp", None)
    row_spec = P(("model", "fsdp"), None)
    weight_spec = P("fsdp", None)

    def device_step(tok_ids, tok_labels, table_shard, gate_shard, up_shard, down_shard, gain_in, gain_out):
        count = tok_ids.shape[0] * tok_ids.shape[1]
        vocab = table_shard.shape[0]
        devices = model_size * fsdp_size
        both = lax.all_gather(jnp.stack([tok_ids.reshape(-1), tok_labels.reshape(-1)]), "fsdp", axis=1, tiled=True)
        ids, labels = lax.sort((both[0], both[1]), num_keys=1)
        sorted_ids = ids.reshape(count, fsdp_size).T
        sorted_labels = labels.reshape(count, fsdp_size).T
        edges = jnp.arange(devices + 1, dtype=jnp.int32) * vocab
        starts = jnp.sum((sorted_ids[:, :, None] < edges[None, None, :]).astype(jnp.int32), axis=1)
        dev_cap = capacity(count * fsdp_size, devices, fsdp_size)
        chip_cap = capacity(count * fsdp_size, model_size, fsdp_size)
        dev_counts = starts[:, 1:] - starts[:, :-1]
        chip_starts = starts[:, ::fsdp_size]
        chip_counts = chip_starts[:, 1:] - chip_starts[:, :-1]
        fits = (jnp.max(dev_counts) <= dev_cap) & (jnp.max(chip_counts) <= chip_cap)
        weights = (table_shard, gate_shard, up_shard, down_shard, gain_in, gain_out)
        return lax.cond(
            fits,
            lambda: fast_step(sorted_ids, sorted_labels, starts, (model_size, fsdp_size, dev_cap, chip_cap), *weights),
            lambda: slow_step(tok_ids, tok_labels, *weights),
        )

    return jax.shard_map(device_step, mesh=mesh, in_specs=(tok_spec, tok_spec, row_spec, weight_spec, weight_spec, weight_spec, P(), P()), out_specs=(P(), row_spec, weight_spec, weight_spec, weight_spec), check_vma=False)
```

```python
import functools

import jax
import jax.numpy as jnp
from jax import lax
from jax.experimental import pallas as pl
from jax.experimental.pallas import tpu as pltpu
from jax.sharding import PartitionSpec as P

EPS = 1e-6
VMEM_LIMIT = 63 * 1024 * 1024
LANES = 128
TN = (((0,), (0,)), ((), ()))
NT = (((1,), (1,)), ((), ()))


def rms_scale(values, gain_vec):
    mean_sq = jnp.mean(values * values, axis=-1, keepdims=True)
    return values * lax.rsqrt(mean_sq + EPS) * gain_vec


def mlp_forward(x_emb, gain_in, w_gate, w_up, w_down):
    normed_in, norm_in_back = jax.vjp(lambda values: rms_scale(values, gain_in), x_emb)
    normed_bf = normed_in.astype(jnp.bfloat16)
    gate_f = jnp.dot(normed_bf, w_gate, preferred_element_type=jnp.float32).astype(jnp.bfloat16).astype(jnp.float32)
    up_f = jnp.dot(normed_bf, w_up, preferred_element_type=jnp.float32).astype(jnp.bfloat16).astype(jnp.float32)
    gate_sig = jax.nn.sigmoid(gate_f)
    silu_gate = gate_f * gate_sig
    act_bf = (silu_gate * up_f).astype(jnp.bfloat16)
    mlp_out = jnp.dot(act_bf, w_down, preferred_element_type=jnp.float32).astype(jnp.bfloat16)
    h_res = x_emb + mlp_out.astype(jnp.float32)
    return h_res, (norm_in_back, normed_bf, gate_f, up_f, gate_sig, silu_gate, act_bf)


def mlp_backward(d_hidden, saved, w_gate, w_up, w_down):
    norm_in_back, normed_bf, gate_f, up_f, gate_sig, silu_gate, act_bf = saved
    d_mlp = d_hidden.astype(jnp.bfloat16)
    d_act = jnp.einsum("td,fd->tf", d_mlp, w_down, preferred_element_type=jnp.float32)
    grad_down = jnp.einsum("tf,td->fd", act_bf, d_mlp, preferred_element_type=jnp.float32)
    d_gate = (d_act * up_f * (gate_sig * (1.0 + gate_f * (1.0 - gate_sig)))).astype(jnp.bfloat16)
    d_up = (d_act * silu_gate).astype(jnp.bfloat16)
    grad_gate = jnp.einsum("td,tf->df", normed_bf, d_gate, preferred_element_type=jnp.float32)
    grad_up = jnp.einsum("td,tf->df", normed_bf, d_up, preferred_element_type=jnp.float32)
    d_normed = jnp.einsum("tf,df->td", d_gate, w_gate, preferred_element_type=jnp.float32) + jnp.einsum("tf,df->td", d_up, w_up, preferred_element_type=jnp.float32)
    d_x = d_hidden + norm_in_back(d_normed)[0]
    return d_x, grad_gate, grad_up, grad_down


def slow_step(tok_ids, tok_labels, halves, table_shard, gain_in, gain_out):
    fsdp_size = lax.axis_size("fsdp")
    local_count = tok_ids.shape[0] * tok_ids.shape[1]
    num_tokens = local_count * fsdp_size
    table_part = lax.all_gather(table_shard, "fsdp", axis=0, tiled=True)
    w_gate, w_up, w_down = (by_core(lax.axis_index("fsdp"), mine, theirs) for mine, theirs in halves)
    vocab_part = table_part.shape[0]
    vocab_start = lax.axis_index("model") * vocab_part
    local_ids = tok_ids.reshape(local_count) - vocab_start
    id_inside = (local_ids >= 0) & (local_ids < vocab_part)
    safe_ids = jnp.where(id_inside, local_ids, 0)
    emb_rows = jnp.where(id_inside[:, None], jnp.take(table_part, safe_ids, axis=0), 0)
    x_emb = lax.psum(emb_rows, "model").astype(jnp.float32)
    h_res, saved = mlp_forward(x_emb, gain_in, w_gate, w_up, w_down)
    hn_f, norm_out_back = jax.vjp(lambda values: rms_scale(values, gain_out), h_res)
    hn_bf = hn_f.astype(jnp.bfloat16)
    logits = jnp.einsum("td,vd->tv", hn_bf, table_part, preferred_element_type=jnp.float32)
    row_max = lax.pmax(jnp.max(logits, axis=-1), "model")
    exp_shift = jnp.exp(logits - row_max[:, None])
    local_labels = tok_labels.reshape(local_count) - vocab_start
    onehot = lax.broadcasted_iota(jnp.int32, logits.shape, 1) == local_labels[:, None]
    part_stats = jnp.stack([jnp.sum(exp_shift, axis=-1), jnp.sum(jnp.where(onehot, logits, 0.0), axis=-1)])
    tok_stats = lax.psum(part_stats, "model")
    sum_exp = tok_stats[0]
    tok_loss = row_max + jnp.log(sum_exp) - tok_stats[1]
    loss = lax.psum(jnp.sum(tok_loss), "fsdp") / num_tokens
    soft_probs = exp_shift / sum_exp[:, None]
    d_logits = (jnp.where(onehot, soft_probs - 1.0, soft_probs) / num_tokens).astype(jnp.bfloat16)
    d_head = jnp.einsum("tv,td->vd", d_logits, hn_bf, preferred_element_type=jnp.float32)
    d_hn = lax.psum(jnp.einsum("tv,vd->td", d_logits, table_part, preferred_element_type=jnp.float32), "model")
    d_hidden = norm_out_back(d_hn)[0]
    d_x, grad_gate, grad_up, grad_down = mlp_backward(d_hidden, saved, w_gate, w_up, w_down)
    d_in = jax.ops.segment_sum(jnp.where(id_inside[:, None], d_x, 0.0), safe_ids, num_segments=vocab_part)
    grad_table = lax.psum_scatter(d_head + d_in, "fsdp", scatter_dimension=0, tiled=True)
    grad_gate = lax.psum_scatter(grad_gate, "fsdp", scatter_dimension=0, tiled=True)
    grad_up = lax.psum_scatter(grad_up, "fsdp", scatter_dimension=0, tiled=True)
    grad_down = lax.psum_scatter(grad_down, "fsdp", scatter_dimension=0, tiled=True)
    return loss, grad_table, grad_gate, grad_up, grad_down


def lane_chunks(width, chunk):
    return [(lo, min(chunk, width - lo)) for lo in range(0, width, chunk)]

def logits_kernel(chunk, hn_ref, emb_ref, off_ref, z_ref, stat_ref):
    rows, vocab = z_ref.shape
    hn = hn_ref[...]
    off = off_ref[...]
    lane = lax.broadcasted_iota(jnp.int32, (rows, LANES), 1)
    run_max = jnp.full((rows, LANES), -jnp.inf, jnp.float32)
    run_sum = jnp.zeros((rows, LANES), jnp.float32)
    run_lab = jnp.zeros((rows, LANES), jnp.float32)
    for lo, width in lane_chunks(vocab, chunk):
        z = lax.dot_general(hn, emb_ref[lo:lo + width, :], NT, preferred_element_type=jnp.float32)
        z_ref[:, lo:lo + width] = z
        groups = width // LANES
        parts = [z[:, g * LANES:(g + 1) * LANES] for g in range(groups)]
        if width % LANES:
            short = width % LANES
            filler = jnp.full((rows, LANES - short), -jnp.inf, jnp.float32)
            parts.append(jnp.concatenate([z[:, groups * LANES:], filler], axis=1))
        new_max = run_max
        for g, part in enumerate(parts):
            new_max = jnp.maximum(new_max, part)
            run_lab = jnp.where(off == -(lo + g * LANES), part, run_lab)
        run_sum = run_sum * jnp.exp(run_max - new_max)
        for part in parts:
            run_sum = run_sum + jnp.exp(part - new_max)
        run_max = new_max
    row_max = jnp.max(run_max, axis=1, keepdims=True)
    row_sum = jnp.sum(run_sum * jnp.exp(run_max - row_max), axis=1, keepdims=True)
    row_lab = jnp.sum(run_lab, axis=1, keepdims=True)
    stat_ref[...] = jnp.where(lane == 0, row_max, jnp.where(lane == 1, row_sum, row_lab))


def head_logits(hn, table, off, blk=256, chunk=1024):
    tokens, depth = hn.shape
    vocab = table.shape[0]
    return pl.pallas_call(
        functools.partial(logits_kernel, chunk),
        grid=(tokens // blk,),
        in_specs=[
            pl.BlockSpec((blk, depth), lambda i: (i, 0)),
            pl.BlockSpec((vocab, depth), lambda i: (0, 0), pipeline_mode=pl.Buffered(1)),
            pl.BlockSpec((blk, LANES), lambda i: (i, 0)),
        ],
        out_specs=[
            pl.BlockSpec((blk, vocab), lambda i: (i, 0)),
            pl.BlockSpec((blk, LANES), lambda i: (i, 0)),
        ],
        out_shape=[jax.ShapeDtypeStruct((tokens, vocab), jnp.float32), jax.ShapeDtypeStruct((tokens, LANES), jnp.float32)],
        cost_estimate=pl.CostEstimate(flops=2 * tokens * vocab * depth, bytes_accessed=4 * tokens * vocab, transcendentals=tokens * vocab),
        compiler_params=pltpu.CompilerParams(vmem_limit_bytes=VMEM_LIMIT),
        name="head_logits",
    )(hn, table, off)


def dlogits_kernel(inv_tokens, chunk, z_ref, emb_ref, max_ref, scale_ref, off_ref, dz_ref, dhn_ref):
    vocab = z_ref.shape[1]
    row_max = max_ref[...]
    scale = scale_ref[...]
    off = off_ref[...]
    total = None
    for lo, width in lane_chunks(vocab, chunk):
        for g in range(0, width, LANES):
            lanes = min(LANES, width - g)
            cols = slice(lo + g, lo + g + lanes)
            grad = jnp.exp(z_ref[:, cols] - row_max[:, :lanes]) * scale[:, :lanes]
            grad = jnp.where(off[:, :lanes] == -(lo + g), grad - inv_tokens, grad)
            dz_ref[:, cols] = grad.astype(jnp.bfloat16)
        part = jnp.dot(dz_ref[:, lo:lo + width], emb_ref[lo:lo + width, :], preferred_element_type=jnp.float32)
        total = part if total is None else total + part
    dhn_ref[...] = total


def head_dlogits(z, table, row_max, scale, off, inv_tokens, cols, blk=512, chunk=1024):
    tokens, vocab = z.shape
    row = pl.BlockSpec((blk, LANES), lambda i: (i, 0))
    return pl.pallas_call(
        functools.partial(dlogits_kernel, inv_tokens, chunk),
        grid=(tokens // blk,),
        in_specs=[
            pl.BlockSpec((blk, vocab), lambda i: (i, 0)),
            pl.BlockSpec((vocab, cols), lambda i: (0, 0), pipeline_mode=pl.Buffered(1)),
            row,
            row,
            row,
        ],
        out_specs=[
            pl.BlockSpec((blk, vocab), lambda i: (i, 0)),
            pl.BlockSpec((blk, cols), lambda i: (i, 0)),
        ],
        out_shape=[jax.ShapeDtypeStruct((tokens, vocab), jnp.bfloat16), jax.ShapeDtypeStruct((tokens, cols), jnp.float32)],
        cost_estimate=pl.CostEstimate(flops=2 * tokens * vocab * cols, bytes_accessed=6 * tokens * vocab, transcendentals=tokens * vocab),
        compiler_params=pltpu.CompilerParams(vmem_limit_bytes=VMEM_LIMIT),
        name="head_dlogits",
    )(z, table, row_max, scale, off)


def dhn_kernel(dz_ref, emb_ref, dhn_ref):
    dhn_ref[...] = jnp.dot(dz_ref[...], emb_ref[...], preferred_element_type=jnp.float32)


def head_dhn(dz, table, cols, index, blk=512):
    tokens, vocab = dz.shape
    return pl.pallas_call(
        dhn_kernel,
        grid=(tokens // blk,),
        in_specs=[
            pl.BlockSpec((blk, vocab), lambda i: (i, 0)),
            pl.BlockSpec((vocab, cols), lambda i: (0, index), pipeline_mode=pl.Buffered(1)),
        ],
        out_specs=pl.BlockSpec((blk, cols), lambda i: (i, 0)),
        out_shape=jax.ShapeDtypeStruct((tokens, cols), jnp.float32),
        cost_estimate=pl.CostEstimate(flops=2 * tokens * vocab * cols, bytes_accessed=2 * tokens * vocab, transcendentals=0),
        compiler_params=pltpu.CompilerParams(vmem_limit_bytes=VMEM_LIMIT),
        name="head_dhn",
    )(dz, table)


def dtable_kernel(a_ref, ha_ref, b_ref, hb_ref, *refs):
    out_ref = refs[-1]
    out_ref[...] = (lax.dot_general(a_ref[...], ha_ref[...], TN, preferred_element_type=jnp.float32)
                    + lax.dot_general(b_ref[...], hb_ref[...], TN, preferred_element_type=jnp.float32))


def head_dtable(dz_a, hn_a, dz_b, hn_b, partial, tile=640, early=0.7):
    tokens, vocab = dz_a.shape
    depth = hn_a.shape[1]
    tiles = pl.cdiv(vocab, tile)
    split = int(early * tiles)
    start, steps = (0, split) if partial is None else (split, tiles - split)
    dz_spec = pl.BlockSpec((tokens, tile), lambda i: (0, i + start))
    hn_spec = pl.BlockSpec((tokens, depth), lambda i: (0, 0), pipeline_mode=pl.Buffered(1))
    rest = () if partial is None else (partial,)
    return pl.pallas_call(
        dtable_kernel,
        grid=(steps,),
        in_specs=[dz_spec, hn_spec, dz_spec, hn_spec] + [pl.BlockSpec(memory_space=pl.ANY)] * len(rest),
        out_specs=pl.BlockSpec((tile, depth), lambda i: (i + start, 0)),
        out_shape=jax.ShapeDtypeStruct((vocab, depth), jnp.float32),
        input_output_aliases={4: 0} if rest else {},
        cost_estimate=pl.CostEstimate(flops=4 * tokens * steps * tile * depth, bytes_accessed=4 * tokens * steps * tile, transcendentals=0),
        compiler_params=pltpu.CompilerParams(vmem_limit_bytes=VMEM_LIMIT),
        name="head_dtable",
    )(dz_a, hn_a, dz_b, hn_b, *rest)


def norm(values, gain):
    return values * lax.rsqrt(jnp.mean(values * values, axis=-1, keepdims=True) + EPS) * gain

def mlp_kernel(chunk, x_ref, g1_ref, g2_ref, wg_ref, wu_ref, wd_ref, a_ref, gt_ref, up_ref, q_ref, h_ref, hn_ref):
    x = x_ref[...]
    a = norm(x, g1_ref[...]).astype(jnp.bfloat16)
    a_ref[...] = a
    total = None
    for lo in range(0, gt_ref.shape[1], chunk):
        cols = slice(lo, lo + chunk)
        gt = jnp.dot(a, wg_ref[:, cols], preferred_element_type=jnp.float32).astype(jnp.bfloat16)
        up = jnp.dot(a, wu_ref[:, cols], preferred_element_type=jnp.float32).astype(jnp.bfloat16)
        gt_ref[:, cols] = gt
        up_ref[:, cols] = up
        gate = gt.astype(jnp.float32)
        q = (gate * jax.nn.sigmoid(gate) * up.astype(jnp.float32)).astype(jnp.bfloat16)
        q_ref[:, cols] = q
        part = jnp.dot(q, wd_ref[cols, :], preferred_element_type=jnp.float32)
        total = part if total is None else total + part
    h = x + total.astype(jnp.bfloat16).astype(jnp.float32)
    h_ref[...] = h
    hn_ref[...] = norm(h, g2_ref[...]).astype(jnp.bfloat16)

def mlp_forward_kernel(x, g1, g2, wg, wu, wd, tokens, blk=256, chunk=1024):
    depth = x.shape[1]
    width = wg.shape[1]
    row = lambda n: pl.BlockSpec((blk, n), lambda i: (i, 0))
    whole = lambda s: pl.BlockSpec(s, lambda i: (0, 0), pipeline_mode=pl.Buffered(1))
    shape = lambda n, t: jax.ShapeDtypeStruct((tokens, n), t)
    return pl.pallas_call(
        functools.partial(mlp_kernel, chunk),
        grid=(tokens // blk,),
        in_specs=[row(depth), whole((1, depth)), whole((1, depth)), whole(wg.shape), whole(wu.shape), whole(wd.shape)],
        out_specs=[row(depth), row(width), row(width), row(width), row(depth), row(depth)],
        out_shape=[shape(depth, jnp.bfloat16), shape(width, jnp.bfloat16), shape(width, jnp.bfloat16), shape(width, jnp.bfloat16), shape(depth, jnp.float32), shape(depth, jnp.bfloat16)],
        cost_estimate=pl.CostEstimate(flops=6 * tokens * width * depth, bytes_accessed=6 * tokens * width, transcendentals=tokens * width),
        compiler_params=pltpu.CompilerParams(vmem_limit_bytes=VMEM_LIMIT),
        name="mlp_forward",
    )(x, g1.reshape(1, -1), g2.reshape(1, -1), wg, wu, wd)

def dact_kernel(chunk, dm_ref, wd_ref, gt_ref, up_ref, dgt_ref, dup_ref):
    dm = dm_ref[...]
    for lo in range(0, gt_ref.shape[1], chunk):
        cols = slice(lo, lo + chunk)
        dq = lax.dot_general(dm, wd_ref[cols, :], NT, preferred_element_type=jnp.float32)
        gate = gt_ref[:, cols].astype(jnp.float32)
        up = up_ref[:, cols].astype(jnp.float32)
        sig = jax.nn.sigmoid(gate)
        dgt_ref[:, cols] = (dq * up * (sig * (1.0 + gate * (1.0 - sig)))).astype(jnp.bfloat16)
        dup_ref[:, cols] = (dq * (gate * sig)).astype(jnp.bfloat16)

def mlp_dact(dm, wd, gt, up, blk=256, chunk=1024):
    tokens, depth = dm.shape
    width = wd.shape[0]
    row = lambda n: pl.BlockSpec((blk, n), lambda i: (i, 0))
    return pl.pallas_call(
        functools.partial(dact_kernel, chunk),
        grid=(tokens // blk,),
        in_specs=[row(depth), pl.BlockSpec(wd.shape, lambda i: (0, 0), pipeline_mode=pl.Buffered(1)), row(width), row(width)],
        out_specs=[row(width), row(width)],
        out_shape=[jax.ShapeDtypeStruct((tokens, width), jnp.bfloat16)] * 2,
        cost_estimate=pl.CostEstimate(flops=2 * tokens * width * depth, bytes_accessed=8 * tokens * width, transcendentals=tokens * width),
        compiler_params=pltpu.CompilerParams(vmem_limit_bytes=VMEM_LIMIT),
        name="mlp_dact",
    )(dm, wd, gt, up)


def add_rows_kernel(bound_ref, ids_ref, base_ref, own_ref, theirs_ref, out_ref):
    tile = pl.program_id(0)
    out_ref[...] = base_ref[...]
    start = tile * out_ref.shape[0]
    for part, rows_ref in enumerate((own_ref, theirs_ref)):
        def body(t, carry, part=part, rows_ref=rows_ref):
            row = ids_ref[part, t] - start
            out_ref[pl.ds(row, 1), :] = out_ref[pl.ds(row, 1), :] + rows_ref[pl.ds(t, 1), :]
            return carry
        lax.fori_loop(bound_ref[part, tile], bound_ref[part, tile + 1], body, 0)


def add_rows(base, own, theirs, ids, bounds, tile):
    vocab, depth = base.shape
    whole = pl.BlockSpec(own.shape, lambda i, *_: (0, 0), pipeline_mode=pl.Buffered(1))
    return pl.pallas_call(
        add_rows_kernel,
        grid_spec=pltpu.PrefetchScalarGridSpec(
            num_scalar_prefetch=2,
            grid=(vocab // tile,),
            in_specs=[pl.BlockSpec((tile, depth), lambda i, *_: (i, 0)), whole, whole],
            out_specs=pl.BlockSpec((tile, depth), lambda i, *_: (i, 0)),
        ),
        out_shape=jax.ShapeDtypeStruct(base.shape, base.dtype),
        input_output_aliases={2: 0},
        cost_estimate=pl.CostEstimate(flops=2 * vocab * depth, bytes_accessed=8 * vocab * depth, transcendentals=0),
        compiler_params=pltpu.CompilerParams(vmem_limit_bytes=VMEM_LIMIT),
        name="add_rows",
    )(bounds, ids, base, own, theirs)


def place_kernel(start_ref, block_ref, out_ref, *scratch):
    rows = scratch[0] if scratch else out_ref
    _, cap, depth = block_ref.shape
    start = start_ref[pl.program_id(0)]
    sub = lax.broadcasted_iota(jnp.int32, (8, depth), 0)
    base = pl.multiple_of(start // 8 * 8, 8)
    shift = start % 8
    before = rows[pl.ds(base, 8), :]
    for j in range(0, cap, 16):
        piece = block_ref[0, j:j + 16, :].astype(jnp.float32)
        for k in (0, 8):
            turned = pltpu.roll(piece[k:k + 8], shift, 0)
            rows[pl.ds(pl.multiple_of(base + (j + k), 8), 8), :] = jnp.where(sub < shift, before, turned)
            before = turned
    tail = pl.ds(pl.multiple_of(base + cap, 8), 8)
    rows[tail, :] = jnp.where(sub < shift, before, rows[tail, :])
    if scratch:
        @pl.when(pl.program_id(0) == pl.num_programs(0) - 1)
        def _():
            out_ref[...] = rows[:out_ref.shape[0]].astype(out_ref.dtype)


def place_rows(blocks, starts, count, dtype):
    number, cap, depth = blocks.shape
    return pl.pallas_call(
        place_kernel,
        grid_spec=pltpu.PrefetchScalarGridSpec(
            num_scalar_prefetch=1,
            grid=(number,),
            in_specs=[pl.BlockSpec((1, cap, depth), lambda b, *_: (b, 0, 0))],
            out_specs=pl.BlockSpec((count, depth), lambda b, *_: (0, 0)),
            scratch_shapes=[] if dtype == jnp.float32 else [pltpu.VMEM((count + 8, depth), jnp.float32)],
        ),
        out_shape=jax.ShapeDtypeStruct((count, depth), dtype),
        cost_estimate=pl.CostEstimate(flops=8 * count * depth, bytes_accessed=8 * count * depth, transcendentals=0),
        compiler_params=pltpu.CompilerParams(vmem_limit_bytes=VMEM_LIMIT),
        name="place_rows",
    )(starts, blocks)


def window_kernel(first_ref, a_ref, b_ref, out_ref):
    count, _ = a_ref.shape
    cap = out_ref.shape[1]
    first = first_ref[pl.program_id(0)]
    base = pl.multiple_of(jnp.minimum(first // 8, (count - cap) // 8 - 1) * 8, 8)
    keep = 8 - (first - base)
    sub = lax.broadcasted_iota(jnp.int32, (8, a_ref.shape[1]), 0)
    here = None
    for j in range(0, cap + 8, 8):
        rows = pl.ds(pl.multiple_of(base + j, 8), 8)
        turned = pltpu.roll(a_ref[rows, :] + b_ref[rows, :], keep % 8, 0)
        if j:
            out_ref[0, j - 8:j, :] = jnp.where(sub < keep, here, turned)
        here = turned


def sum_windows(a, b, first, cap):
    count, depth = a.shape
    whole = pl.BlockSpec((count, depth), lambda c, *_: (0, 0), pipeline_mode=pl.Buffered(1))
    return pl.pallas_call(
        window_kernel,
        grid_spec=pltpu.PrefetchScalarGridSpec(
            num_scalar_prefetch=1,
            grid=(first.shape[0],),
            in_specs=[whole, whole],
            out_specs=pl.BlockSpec((1, cap, depth), lambda c, *_: (c, 0, 0)),
        ),
        out_shape=jax.ShapeDtypeStruct((first.shape[0], cap, depth), jnp.float32),
        cost_estimate=pl.CostEstimate(flops=8 * a.size, bytes_accessed=12 * a.size, transcendentals=0),
        compiler_params=pltpu.CompilerParams(vmem_limit_bytes=VMEM_LIMIT),
        name="sum_windows",
    )(first, a, b)


def swap_cores(values):
    return lax.ppermute(values, "fsdp", [(0, 1), (1, 0)])


def by_core(core, mine, theirs):
    return jnp.where(core == 0, jnp.concatenate([mine, theirs]), jnp.concatenate([theirs, mine]))


def owned_rows(sorted_ids, starts, dev_cap, table_shard):
    vocab, depth = table_shard.shape
    core = lax.axis_index("fsdp")
    device = lax.axis_index("model") * sorted_ids.shape[0] + core
    padded = jnp.pad(sorted_ids, ((0, 0), (0, dev_cap)))
    first = lax.dynamic_index_in_dim(starts, device, 1, keepdims=False)
    ids = jnp.concatenate([lax.dynamic_slice(padded, (part, first[part]), (1, dev_cap))[0] for part in (1 - core, core)])
    rows = jnp.take(table_shard, jnp.clip(ids - device * vocab, 0, vocab - 1), axis=0, mode="clip")
    theirs = swap_cores(rows[:dev_cap])
    return by_core(core, rows[dev_cap:], theirs).reshape(2, dev_cap, depth)


def fast_step(sorted_ids, sorted_labels, starts, sizes, pair, halves, table_shard, gain_in, gain_out):
    model_size, fsdp_size, dev_cap, chip_cap = sizes
    vocab, depth = table_shard.shape
    chip = lax.axis_index("model")
    core = lax.axis_index("fsdp")
    device = chip * fsdp_size + core
    count = sorted_ids.shape[1]
    num_tokens = count * fsdp_size
    half = depth // 2
    own = lambda values: lax.dynamic_index_in_dim(values, core, 0, keepdims=False)
    other = lambda values: lax.dynamic_index_in_dim(values, 1 - core, 0, keepdims=False)

    my_starts = own(starts)
    blocks = lax.all_gather(pair, "model", axis=0, tiled=True)
    w_gate, w_up, w_down = (by_core(core, mine, theirs) for mine, theirs in halves)
    x_buf = place_rows(blocks, my_starts, count + dev_cap + 8, jnp.float32)
    normed_bf, gate_bf, up_bf, act_bf, h_res, hn_own = mlp_forward_kernel(x_buf, gain_in, gain_out, w_gate, w_up, w_down, count)
    hn_other = swap_cores(hn_own)
    lane = lax.broadcasted_iota(jnp.int32, (fsdp_size, count, LANES), 2)
    local_labels = (sorted_labels - device * vocab)[:, :, None]
    offs = jnp.where((local_labels >= 0) & (local_labels < vocab), lane - local_labels, 1)
    off_own, off_other = own(offs), other(offs)
    z_own, stat_own = head_logits(hn_own, table_shard, off_own)
    z_other, stat_other = head_logits(hn_other, table_shard, off_other)
    part = by_core(core, stat_own[:, :3].T, stat_other[:, :3].T)
    all_stats = lax.all_gather(part, ("model", "fsdp"), axis=0).reshape(-1, fsdp_size, 3, count)
    row_max = jnp.max(all_stats[:, :, 0], axis=0)
    sum_exp = jnp.sum(all_stats[:, :, 1] * jnp.exp(all_stats[:, :, 0] - row_max[None]), axis=0)
    label_logit = jnp.sum(all_stats[:, :, 2], axis=0)
    loss = jnp.sum(row_max + jnp.log(sum_exp) - label_logit) / num_tokens
    max_lanes = jnp.broadcast_to(row_max[:, :, None], (fsdp_size, count, LANES))
    scale_lanes = jnp.broadcast_to((1.0 / sum_exp / num_tokens)[:, :, None], (fsdp_size, count, LANES))
    inv_tokens = 1.0 / num_tokens
    dz_other, d_hn_other = head_dlogits(z_other, table_shard, other(max_lanes), other(scale_lanes), off_other, inv_tokens, half)
    d_hn_theirs = swap_cores(d_hn_other)
    dz_own, d_hn_own = head_dlogits(z_own, table_shard, own(max_lanes), own(scale_lanes), off_own, inv_tokens, half)

    first = jnp.minimum(my_starts[0:model_size * fsdp_size:fsdp_size], count - chip_cap)
    windows = sum_windows(d_hn_own, d_hn_theirs, first, chip_cap)
    windows, dz_other, dz_own = lax.optimization_barrier((windows, dz_other, dz_own))
    d_hn_left = lax.psum_scatter(windows.reshape(model_size * chip_cap, half), "model", scatter_dimension=0, tiled=True)
    d_hn_other = head_dhn(dz_other, table_shard, half, 1)
    d_hn_theirs = swap_cores(d_hn_other)
    d_hn_own = head_dhn(dz_own, table_shard, half, 1)
    windows = sum_windows(d_hn_own, d_hn_theirs, first, chip_cap)
    windows, dz_other, dz_own = lax.optimization_barrier((windows, dz_other, dz_own))
    d_hn_right = lax.psum_scatter(windows.reshape(model_size * chip_cap, half), "model", scatter_dimension=0, tiled=True)
    d_head = head_dtable(dz_own, hn_own, dz_other, hn_other, None)
    d_hn_left, d_hn_right, d_head = lax.optimization_barrier((d_hn_left, d_hn_right, d_head))
    d_hn = jnp.concatenate([d_hn_left, d_hn_right], axis=1)
    my_first = lax.dynamic_index_in_dim(first, chip, 0, keepdims=False)
    h_window = lax.dynamic_slice(h_res, (my_first, 0), (chip_cap, depth))
    _, norm_out_back = jax.vjp(lambda values: rms_scale(values, gain_out), h_window)
    d_hidden = norm_out_back(d_hn)[0]
    dm_blocks = lax.all_gather(d_hidden.astype(jnp.bfloat16), "model", axis=0)
    d_head = head_dtable(dz_own, hn_own, dz_other, hn_other, d_head)
    dm_blocks, d_head = lax.optimization_barrier((dm_blocks, d_head))
    d_mlp = place_rows(dm_blocks, first, count, jnp.bfloat16)

    d_gate, d_up = mlp_dact(d_mlp, w_down, gate_bf, up_bf)
    grad_down = jnp.einsum("tf,td->fd", act_bf, d_mlp, preferred_element_type=jnp.float32)
    grad_gate = jnp.einsum("td,tf->df", normed_bf, d_gate, preferred_element_type=jnp.float32)
    grad_up = jnp.einsum("td,tf->df", normed_bf, d_up, preferred_element_type=jnp.float32)
    d_gate_own = lax.dynamic_slice(d_gate, (my_first, 0), (chip_cap, d_gate.shape[1]))
    d_up_own = lax.dynamic_slice(d_up, (my_first, 0), (chip_cap, d_up.shape[1]))
    x_window = lax.dynamic_slice(x_buf, (my_first, 0), (chip_cap, depth))
    d_normed = jnp.einsum("tf,df->td", d_gate_own, w_gate, preferred_element_type=jnp.float32) + jnp.einsum("tf,df->td", d_up_own, w_up, preferred_element_type=jnp.float32)
    _, norm_in_back = jax.vjp(lambda values: rms_scale(values, gain_in), x_window)
    d_x = d_hidden + norm_in_back(d_normed)[0]
    d_x_theirs = swap_cores(d_x)

    tile = vocab // 6
    pair_first = jnp.minimum(lax.dynamic_index_in_dim(starts, chip * fsdp_size, 1, keepdims=False), count - chip_cap)
    own_ids = jnp.stack([lax.dynamic_slice(sorted_ids, (p, pair_first[p]), (1, chip_cap))[0] for p in (core, 1 - core)]) - device * vocab
    edges = jnp.arange(vocab // tile + 1, dtype=jnp.int32) * tile
    bounds = jnp.sum((own_ids[:, :, None] < edges[None, None, :]).astype(jnp.int32), axis=1)
    grad_table = add_rows(d_head, d_x, d_x_theirs, own_ids, bounds, tile)

    grad_gate = lax.psum_scatter(grad_gate, "fsdp", scatter_dimension=0, tiled=True)
    grad_up = lax.psum_scatter(grad_up, "fsdp", scatter_dimension=0, tiled=True)
    grad_down = lax.psum_scatter(grad_down, "fsdp", scatter_dimension=0, tiled=True)
    return loss, grad_table, grad_gate, grad_up, grad_down


def capacity(tokens, shares, lists):
    mean = tokens / shares
    deviation = (mean * (1 - 1 / shares)) ** 0.5
    return -(-int((mean + 4.5 * deviation) / lists) // 16) * 16


def solution(mesh):
    fsdp_size = mesh.shape["fsdp"]
    model_size = mesh.shape["model"]
    tok_spec = P("fsdp", None)
    row_spec = P(("model", "fsdp"), None)
    weight_spec = P("fsdp", None)

    def device_step(tok_ids, tok_labels, table_shard, gate_shard, up_shard, down_shard, gain_in, gain_out):
        count = tok_ids.shape[0] * tok_ids.shape[1]
        vocab = table_shard.shape[0]
        devices = model_size * fsdp_size
        both = lax.all_gather(jnp.stack([tok_ids.reshape(-1), tok_labels.reshape(-1)]), "fsdp", axis=1, tiled=True)
        both, gate_shard, up_shard, down_shard = lax.optimization_barrier((both, gate_shard, up_shard, down_shard))
        ids, labels = lax.sort((both[0], both[1]), num_keys=1)
        sorted_ids = ids.reshape(count, fsdp_size).T
        sorted_labels = labels.reshape(count, fsdp_size).T
        edges = jnp.arange(devices + 1, dtype=jnp.int32) * vocab
        starts = jnp.sum((sorted_ids[:, :, None] < edges[None, None, :]).astype(jnp.int32), axis=1)
        dev_cap = capacity(count * fsdp_size, devices, fsdp_size)
        chip_cap = capacity(count * fsdp_size, model_size, fsdp_size)
        dev_counts = starts[:, 1:] - starts[:, :-1]
        chip_starts = starts[:, ::fsdp_size]
        chip_counts = chip_starts[:, 1:] - chip_starts[:, :-1]
        fits = (jnp.max(dev_counts) <= dev_cap) & (jnp.max(chip_counts) <= chip_cap)
        core = lax.axis_index("fsdp")
        pair = owned_rows(sorted_ids, starts, dev_cap, table_shard)
        halves = tuple((shard, swap_cores(shard)) for shard in (gate_shard, up_shard, down_shard))
        weights = (halves, table_shard, gain_in, gain_out)
        return lax.cond(
            fits,
            lambda: fast_step(sorted_ids, sorted_labels, starts, (model_size, fsdp_size, dev_cap, chip_cap), pair, *weights),
            lambda: slow_step(tok_ids, tok_labels, *weights),
        )

    return jax.shard_map(device_step, mesh=mesh, in_specs=(tok_spec, tok_spec, row_spec, weight_spec, weight_spec, weight_spec, P(), P()), out_specs=(P(), row_spec, weight_spec, weight_spec, weight_spec), check_vma=False)
```

```python
import functools

import jax
import jax.numpy as jnp
from jax import lax
from jax.experimental import pallas as pl
from jax.experimental.pallas import tpu as pltpu
from jax.sharding import PartitionSpec as P

EPS = 1e-6
VMEM_LIMIT = 63 * 1024 * 1024
LANES = 128
NN = (((1,), (0,)), ((), ()))
TN = (((0,), (0,)), ((), ()))
NT = (((1,), (1,)), ((), ()))


def rms_scale(values, gain_vec):
    mean_sq = jnp.mean(values * values, axis=-1, keepdims=True)
    return values * lax.rsqrt(mean_sq + EPS) * gain_vec


def mlp_forward(x_emb, gain_in, w_gate, w_up, w_down):
    normed_in, norm_in_back = jax.vjp(lambda values: rms_scale(values, gain_in), x_emb)
    normed_bf = normed_in.astype(jnp.bfloat16)
    gate_f = jnp.dot(normed_bf, w_gate, preferred_element_type=jnp.float32).astype(jnp.bfloat16).astype(jnp.float32)
    up_f = jnp.dot(normed_bf, w_up, preferred_element_type=jnp.float32).astype(jnp.bfloat16).astype(jnp.float32)
    gate_sig = jax.nn.sigmoid(gate_f)
    silu_gate = gate_f * gate_sig
    act_bf = (silu_gate * up_f).astype(jnp.bfloat16)
    mlp_out = jnp.dot(act_bf, w_down, preferred_element_type=jnp.float32).astype(jnp.bfloat16)
    h_res = x_emb + mlp_out.astype(jnp.float32)
    return h_res, (norm_in_back, normed_bf, gate_f, up_f, gate_sig, silu_gate, act_bf)


def mlp_backward(d_hidden, saved, w_gate, w_up, w_down):
    norm_in_back, normed_bf, gate_f, up_f, gate_sig, silu_gate, act_bf = saved
    d_mlp = d_hidden.astype(jnp.bfloat16)
    d_act = jnp.einsum("td,fd->tf", d_mlp, w_down, preferred_element_type=jnp.float32)
    grad_down = jnp.einsum("tf,td->fd", act_bf, d_mlp, preferred_element_type=jnp.float32)
    d_gate = (d_act * up_f * (gate_sig * (1.0 + gate_f * (1.0 - gate_sig)))).astype(jnp.bfloat16)
    d_up = (d_act * silu_gate).astype(jnp.bfloat16)
    grad_gate = jnp.einsum("td,tf->df", normed_bf, d_gate, preferred_element_type=jnp.float32)
    grad_up = jnp.einsum("td,tf->df", normed_bf, d_up, preferred_element_type=jnp.float32)
    d_normed = jnp.einsum("tf,df->td", d_gate, w_gate, preferred_element_type=jnp.float32) + jnp.einsum("tf,df->td", d_up, w_up, preferred_element_type=jnp.float32)
    d_x = d_hidden + norm_in_back(d_normed)[0]
    return d_x, grad_gate, grad_up, grad_down


def slow_step(tok_ids, tok_labels, halves, table_shard, gain_in, gain_out):
    fsdp_size = lax.axis_size("fsdp")
    local_count = tok_ids.shape[0] * tok_ids.shape[1]
    num_tokens = local_count * fsdp_size
    table_part = lax.all_gather(table_shard, "fsdp", axis=0, tiled=True)
    w_gate, w_up, w_down = (by_core(lax.axis_index("fsdp"), mine, theirs) for mine, theirs in halves)
    vocab_part = table_part.shape[0]
    vocab_start = lax.axis_index("model") * vocab_part
    local_ids = tok_ids.reshape(local_count) - vocab_start
    id_inside = (local_ids >= 0) & (local_ids < vocab_part)
    safe_ids = jnp.where(id_inside, local_ids, 0)
    emb_rows = jnp.where(id_inside[:, None], jnp.take(table_part, safe_ids, axis=0), 0)
    x_emb = lax.psum(emb_rows, "model").astype(jnp.float32)
    h_res, saved = mlp_forward(x_emb, gain_in, w_gate, w_up, w_down)
    hn_f, norm_out_back = jax.vjp(lambda values: rms_scale(values, gain_out), h_res)
    hn_bf = hn_f.astype(jnp.bfloat16)
    logits = jnp.einsum("td,vd->tv", hn_bf, table_part, preferred_element_type=jnp.float32)
    row_max = lax.pmax(jnp.max(logits, axis=-1), "model")
    exp_shift = jnp.exp(logits - row_max[:, None])
    local_labels = tok_labels.reshape(local_count) - vocab_start
    onehot = lax.broadcasted_iota(jnp.int32, logits.shape, 1) == local_labels[:, None]
    part_stats = jnp.stack([jnp.sum(exp_shift, axis=-1), jnp.sum(jnp.where(onehot, logits, 0.0), axis=-1)])
    tok_stats = lax.psum(part_stats, "model")
    sum_exp = tok_stats[0]
    tok_loss = row_max + jnp.log(sum_exp) - tok_stats[1]
    loss = lax.psum(jnp.sum(tok_loss), "fsdp") / num_tokens
    soft_probs = exp_shift / sum_exp[:, None]
    d_logits = (jnp.where(onehot, soft_probs - 1.0, soft_probs) / num_tokens).astype(jnp.bfloat16)
    d_head = jnp.einsum("tv,td->vd", d_logits, hn_bf, preferred_element_type=jnp.float32)
    d_hn = lax.psum(jnp.einsum("tv,vd->td", d_logits, table_part, preferred_element_type=jnp.float32), "model")
    d_hidden = norm_out_back(d_hn)[0]
    d_x, grad_gate, grad_up, grad_down = mlp_backward(d_hidden, saved, w_gate, w_up, w_down)
    d_in = jax.ops.segment_sum(jnp.where(id_inside[:, None], d_x, 0.0), safe_ids, num_segments=vocab_part)
    grad_table = lax.psum_scatter(d_head + d_in, "fsdp", scatter_dimension=0, tiled=True)
    grad_gate = lax.psum_scatter(grad_gate, "fsdp", scatter_dimension=0, tiled=True)
    grad_up = lax.psum_scatter(grad_up, "fsdp", scatter_dimension=0, tiled=True)
    grad_down = lax.psum_scatter(grad_down, "fsdp", scatter_dimension=0, tiled=True)
    return loss, grad_table, grad_gate, grad_up, grad_down


def lane_chunks(width, chunk):
    return [(lo, min(chunk, width - lo)) for lo in range(0, width, chunk)]

def logits_kernel(chunk, hn_ref, emb_ref, off_ref, z_ref, stat_ref):
    rows, vocab = z_ref.shape
    hn = hn_ref[...]
    off = off_ref[...]
    lane = lax.broadcasted_iota(jnp.int32, (rows, LANES), 1)
    run_max = jnp.full((rows, LANES), -jnp.inf, jnp.float32)
    run_sum = jnp.zeros((rows, LANES), jnp.float32)
    run_lab = jnp.zeros((rows, LANES), jnp.float32)
    for lo, width in lane_chunks(vocab, chunk):
        z = lax.dot_general(hn, emb_ref[:, lo:lo + width], NN, preferred_element_type=jnp.float32)
        z_ref[:, lo:lo + width] = z
        groups = width // LANES
        parts = [z[:, g * LANES:(g + 1) * LANES] for g in range(groups)]
        if width % LANES:
            short = width % LANES
            filler = jnp.full((rows, LANES - short), -jnp.inf, jnp.float32)
            parts.append(jnp.concatenate([z[:, groups * LANES:], filler], axis=1))
        new_max = run_max
        for g, part in enumerate(parts):
            new_max = jnp.maximum(new_max, part)
            run_lab = jnp.where(off == -(lo + g * LANES), part, run_lab)
        run_sum = run_sum * jnp.exp(run_max - new_max)
        for part in parts:
            run_sum = run_sum + jnp.exp(part - new_max)
        run_max = new_max
    row_max = jnp.max(run_max, axis=1, keepdims=True)
    row_sum = jnp.sum(run_sum * jnp.exp(run_max - row_max), axis=1, keepdims=True)
    row_lab = jnp.sum(run_lab, axis=1, keepdims=True)
    stat_ref[...] = jnp.where(lane == 0, row_max, jnp.where(lane == 1, row_sum, row_lab))


def head_logits(hn, table_t, off, blk=256, chunk=1024):
    tokens, depth = hn.shape
    vocab = table_t.shape[1]
    return pl.pallas_call(
        functools.partial(logits_kernel, chunk),
        grid=(tokens // blk,),
        in_specs=[
            pl.BlockSpec((blk, depth), lambda i: (i, 0)),
            pl.BlockSpec((depth, vocab), lambda i: (0, 0), pipeline_mode=pl.Buffered(1)),
            pl.BlockSpec((blk, LANES), lambda i: (i, 0)),
        ],
        out_specs=[
            pl.BlockSpec((blk, vocab), lambda i: (i, 0)),
            pl.BlockSpec((blk, LANES), lambda i: (i, 0)),
        ],
        out_shape=[jax.ShapeDtypeStruct((tokens, vocab), jnp.float32), jax.ShapeDtypeStruct((tokens, LANES), jnp.float32)],
        cost_estimate=pl.CostEstimate(flops=2 * tokens * vocab * depth, bytes_accessed=4 * tokens * vocab, transcendentals=tokens * vocab),
        compiler_params=pltpu.CompilerParams(vmem_limit_bytes=VMEM_LIMIT),
        name="head_logits",
    )(hn, table_t, off)


def dlogits_kernel(inv_tokens, chunk, z_ref, emb_ref, max_ref, scale_ref, off_ref, dz_ref, dhn_ref):
    vocab = z_ref.shape[1]
    row_max = max_ref[...]
    scale = scale_ref[...]
    off = off_ref[...]
    total = None
    for lo, width in lane_chunks(vocab, chunk):
        for g in range(0, width, LANES):
            lanes = min(LANES, width - g)
            cols = slice(lo + g, lo + g + lanes)
            grad = jnp.exp(z_ref[:, cols] - row_max[:, :lanes]) * scale[:, :lanes]
            grad = jnp.where(off[:, :lanes] == -(lo + g), grad - inv_tokens, grad)
            dz_ref[:, cols] = grad.astype(jnp.bfloat16)
        part = jnp.dot(dz_ref[:, lo:lo + width], emb_ref[lo:lo + width, :], preferred_element_type=jnp.float32)
        total = part if total is None else total + part
    dhn_ref[...] = total


def head_dlogits(z, table, row_max, scale, off, inv_tokens, cols, blk=512, chunk=1024):
    tokens, vocab = z.shape
    row = pl.BlockSpec((blk, LANES), lambda i: (i, 0))
    return pl.pallas_call(
        functools.partial(dlogits_kernel, inv_tokens, chunk),
        grid=(tokens // blk,),
        in_specs=[
            pl.BlockSpec((blk, vocab), lambda i: (i, 0)),
            pl.BlockSpec((vocab, cols), lambda i: (0, 0), pipeline_mode=pl.Buffered(1)),
            row,
            row,
            row,
        ],
        out_specs=[
            pl.BlockSpec((blk, vocab), lambda i: (i, 0)),
            pl.BlockSpec((blk, cols), lambda i: (i, 0)),
        ],
        out_shape=[jax.ShapeDtypeStruct((tokens, vocab), jnp.bfloat16), jax.ShapeDtypeStruct((tokens, cols), jnp.float32)],
        cost_estimate=pl.CostEstimate(flops=2 * tokens * vocab * cols, bytes_accessed=6 * tokens * vocab, transcendentals=tokens * vocab),
        compiler_params=pltpu.CompilerParams(vmem_limit_bytes=VMEM_LIMIT),
        name="head_dlogits",
    )(z, table, row_max, scale, off)


def dhn_kernel(dz_ref, emb_ref, dhn_ref):
    dhn_ref[...] = jnp.dot(dz_ref[...], emb_ref[...], preferred_element_type=jnp.float32)


def head_dhn(dz, table, cols, index, blk=512):
    tokens, vocab = dz.shape
    return pl.pallas_call(
        dhn_kernel,
        grid=(tokens // blk,),
        in_specs=[
            pl.BlockSpec((blk, vocab), lambda i: (i, 0)),
            pl.BlockSpec((vocab, cols), lambda i: (0, index), pipeline_mode=pl.Buffered(1)),
        ],
        out_specs=pl.BlockSpec((blk, cols), lambda i: (i, 0)),
        out_shape=jax.ShapeDtypeStruct((tokens, cols), jnp.float32),
        cost_estimate=pl.CostEstimate(flops=2 * tokens * vocab * cols, bytes_accessed=2 * tokens * vocab, transcendentals=0),
        compiler_params=pltpu.CompilerParams(vmem_limit_bytes=VMEM_LIMIT),
        name="head_dhn",
    )(dz, table)


def dtable_kernel(a_ref, ha_ref, b_ref, hb_ref, *refs):
    out_ref = refs[-1]
    out_ref[...] = (lax.dot_general(a_ref[...], ha_ref[...], TN, preferred_element_type=jnp.float32)
                    + lax.dot_general(b_ref[...], hb_ref[...], TN, preferred_element_type=jnp.float32))


def head_dtable(dz_a, hn_a, dz_b, hn_b, partial, tile=640, early=0.7):
    tokens, vocab = dz_a.shape
    depth = hn_a.shape[1]
    tiles = pl.cdiv(vocab, tile)
    split = int(early * tiles)
    start, steps = (0, split) if partial is None else (split, tiles - split)
    dz_spec = pl.BlockSpec((tokens, tile), lambda i: (0, i + start))
    hn_spec = pl.BlockSpec((tokens, depth), lambda i: (0, 0), pipeline_mode=pl.Buffered(1))
    rest = () if partial is None else (partial,)
    return pl.pallas_call(
        dtable_kernel,
        grid=(steps,),
        in_specs=[dz_spec, hn_spec, dz_spec, hn_spec] + [pl.BlockSpec(memory_space=pl.ANY)] * len(rest),
        out_specs=pl.BlockSpec((tile, depth), lambda i: (i + start, 0)),
        out_shape=jax.ShapeDtypeStruct((vocab, depth), jnp.float32),
        input_output_aliases={4: 0} if rest else {},
        cost_estimate=pl.CostEstimate(flops=4 * tokens * steps * tile * depth, bytes_accessed=4 * tokens * steps * tile, transcendentals=0),
        compiler_params=pltpu.CompilerParams(vmem_limit_bytes=VMEM_LIMIT),
        name="head_dtable",
    )(dz_a, hn_a, dz_b, hn_b, *rest)


def norm(values, gain):
    return values * lax.rsqrt(jnp.mean(values * values, axis=-1, keepdims=True) + EPS) * gain

def mlp_kernel(chunk, x_ref, g1_ref, g2_ref, wg_ref, wu_ref, wd_ref, a_ref, gt_ref, up_ref, q_ref, h_ref, hn_ref):
    x = x_ref[...]
    a = norm(x, g1_ref[...]).astype(jnp.bfloat16)
    a_ref[...] = a
    total = None
    for lo in range(0, gt_ref.shape[1], chunk):
        cols = slice(lo, lo + chunk)
        gt = jnp.dot(a, wg_ref[:, cols], preferred_element_type=jnp.float32).astype(jnp.bfloat16)
        up = jnp.dot(a, wu_ref[:, cols], preferred_element_type=jnp.float32).astype(jnp.bfloat16)
        gt_ref[:, cols] = gt
        up_ref[:, cols] = up
        gate = gt.astype(jnp.float32)
        q = (gate * jax.nn.sigmoid(gate) * up.astype(jnp.float32)).astype(jnp.bfloat16)
        q_ref[:, cols] = q
        part = jnp.dot(q, wd_ref[cols, :], preferred_element_type=jnp.float32)
        total = part if total is None else total + part
    h = x + total.astype(jnp.bfloat16).astype(jnp.float32)
    h_ref[...] = h
    hn_ref[...] = norm(h, g2_ref[...]).astype(jnp.bfloat16)

def mlp_forward_kernel(x, g1, g2, wg, wu, wd, tokens, blk=256, chunk=1024):
    depth = x.shape[1]
    width = wg.shape[1]
    row = lambda n: pl.BlockSpec((blk, n), lambda i: (i, 0))
    whole = lambda s: pl.BlockSpec(s, lambda i: (0, 0), pipeline_mode=pl.Buffered(1))
    shape = lambda n, t: jax.ShapeDtypeStruct((tokens, n), t)
    return pl.pallas_call(
        functools.partial(mlp_kernel, chunk),
        grid=(tokens // blk,),
        in_specs=[row(depth), whole((1, depth)), whole((1, depth)), whole(wg.shape), whole(wu.shape), whole(wd.shape)],
        out_specs=[row(depth), row(width), row(width), row(width), row(depth), row(depth)],
        out_shape=[shape(depth, jnp.bfloat16), shape(width, jnp.bfloat16), shape(width, jnp.bfloat16), shape(width, jnp.bfloat16), shape(depth, jnp.float32), shape(depth, jnp.bfloat16)],
        cost_estimate=pl.CostEstimate(flops=6 * tokens * width * depth, bytes_accessed=6 * tokens * width, transcendentals=tokens * width),
        compiler_params=pltpu.CompilerParams(vmem_limit_bytes=VMEM_LIMIT),
        name="mlp_forward",
    )(x, g1.reshape(1, -1), g2.reshape(1, -1), wg, wu, wd)

def dact_kernel(rows, dm_ref, wd_ref, gt_ref, up_ref, q_ref, dgt_ref, dup_ref, dwd_ref):
    for lo in range(0, dm_ref.shape[0], rows):
        part = slice(lo, lo + rows)
        dq = lax.dot_general(dm_ref[part, :], wd_ref[...], NT, preferred_element_type=jnp.float32)
        gate = gt_ref[part, :].astype(jnp.float32)
        up = up_ref[part, :].astype(jnp.float32)
        sig = jax.nn.sigmoid(gate)
        dgt_ref[part, :] = (dq * up * (sig * (1.0 + gate * (1.0 - sig)))).astype(jnp.bfloat16)
        dup_ref[part, :] = (dq * (gate * sig)).astype(jnp.bfloat16)
    dwd_ref[...] = lax.dot_general(q_ref[...], dm_ref[...], TN, preferred_element_type=jnp.float32)


def mlp_dact(dm, wd, gt, up, q, cols=512, rows=512):
    tokens, depth = dm.shape
    width = wd.shape[0]
    col = pl.BlockSpec((tokens, cols), lambda j: (0, j))
    row = pl.BlockSpec((cols, depth), lambda j: (j, 0))
    return pl.pallas_call(
        functools.partial(dact_kernel, rows),
        grid=(width // cols,),
        in_specs=[pl.BlockSpec((tokens, depth), lambda j: (0, 0), pipeline_mode=pl.Buffered(1)), row, col, col, col],
        out_specs=[col, col, row],
        out_shape=[jax.ShapeDtypeStruct((tokens, width), jnp.bfloat16)] * 2 + [jax.ShapeDtypeStruct((width, depth), jnp.float32)],
        cost_estimate=pl.CostEstimate(flops=4 * tokens * width * depth, bytes_accessed=10 * tokens * width, transcendentals=tokens * width),
        compiler_params=pltpu.CompilerParams(vmem_limit_bytes=VMEM_LIMIT),
        name="mlp_dact",
    )(dm, wd, gt, up, q)


def add_rows_kernel(bound_ref, ids_ref, base_ref, own_ref, theirs_ref, out_ref):
    tile = pl.program_id(0)
    out_ref[...] = base_ref[...]
    start = tile * out_ref.shape[0]
    for part, rows_ref in enumerate((own_ref, theirs_ref)):
        def body(t, carry, part=part, rows_ref=rows_ref):
            row = ids_ref[part, t] - start
            out_ref[pl.ds(row, 1), :] = out_ref[pl.ds(row, 1), :] + rows_ref[pl.ds(t, 1), :]
            return carry
        lax.fori_loop(bound_ref[part, tile], bound_ref[part, tile + 1], body, 0)


def add_rows(base, own, theirs, ids, bounds, tile):
    vocab, depth = base.shape
    whole = pl.BlockSpec(own.shape, lambda i, *_: (0, 0), pipeline_mode=pl.Buffered(1))
    return pl.pallas_call(
        add_rows_kernel,
        grid_spec=pltpu.PrefetchScalarGridSpec(
            num_scalar_prefetch=2,
            grid=(vocab // tile,),
            in_specs=[pl.BlockSpec((tile, depth), lambda i, *_: (i, 0)), whole, whole],
            out_specs=pl.BlockSpec((tile, depth), lambda i, *_: (i, 0)),
        ),
        out_shape=jax.ShapeDtypeStruct(base.shape, base.dtype),
        input_output_aliases={2: 0},
        cost_estimate=pl.CostEstimate(flops=2 * vocab * depth, bytes_accessed=8 * vocab * depth, transcendentals=0),
        compiler_params=pltpu.CompilerParams(vmem_limit_bytes=VMEM_LIMIT),
        name="add_rows",
    )(bounds, ids, base, own, theirs)


def place_kernel(start_ref, block_ref, out_ref, *scratch):
    rows = scratch[0] if scratch else out_ref
    _, cap, depth = block_ref.shape
    start = start_ref[pl.program_id(0)]
    sub = lax.broadcasted_iota(jnp.int32, (8, depth), 0)
    base = pl.multiple_of(start // 8 * 8, 8)
    shift = start % 8
    before = rows[pl.ds(base, 8), :]
    for j in range(0, cap, 16):
        piece = block_ref[0, j:j + 16, :].astype(jnp.float32)
        for k in (0, 8):
            turned = pltpu.roll(piece[k:k + 8], shift, 0)
            rows[pl.ds(pl.multiple_of(base + (j + k), 8), 8), :] = jnp.where(sub < shift, before, turned)
            before = turned
    tail = pl.ds(pl.multiple_of(base + cap, 8), 8)
    rows[tail, :] = jnp.where(sub < shift, before, rows[tail, :])
    if scratch:
        @pl.when(pl.program_id(0) == pl.num_programs(0) - 1)
        def _():
            out_ref[...] = rows[:out_ref.shape[0]].astype(out_ref.dtype)


def place_rows(blocks, starts, count, dtype):
    number, cap, depth = blocks.shape
    return pl.pallas_call(
        place_kernel,
        grid_spec=pltpu.PrefetchScalarGridSpec(
            num_scalar_prefetch=1,
            grid=(number,),
            in_specs=[pl.BlockSpec((1, cap, depth), lambda b, *_: (b, 0, 0))],
            out_specs=pl.BlockSpec((count, depth), lambda b, *_: (0, 0)),
            scratch_shapes=[] if dtype == jnp.float32 else [pltpu.VMEM((count + 8, depth), jnp.float32)],
        ),
        out_shape=jax.ShapeDtypeStruct((count, depth), dtype),
        cost_estimate=pl.CostEstimate(flops=8 * count * depth, bytes_accessed=8 * count * depth, transcendentals=0),
        compiler_params=pltpu.CompilerParams(vmem_limit_bytes=VMEM_LIMIT),
        name="place_rows",
    )(starts, blocks)


def window_kernel(first_ref, a_ref, b_ref, out_ref):
    count, _ = a_ref.shape
    cap = out_ref.shape[1]
    first = first_ref[pl.program_id(0)]
    base = pl.multiple_of(jnp.minimum(first // 8, (count - cap) // 8 - 1) * 8, 8)
    keep = 8 - (first - base)
    sub = lax.broadcasted_iota(jnp.int32, (8, a_ref.shape[1]), 0)
    here = None
    for j in range(0, cap + 8, 8):
        rows = pl.ds(pl.multiple_of(base + j, 8), 8)
        turned = pltpu.roll(a_ref[rows, :] + b_ref[rows, :], keep % 8, 0)
        if j:
            out_ref[0, j - 8:j, :] = jnp.where(sub < keep, here, turned)
        here = turned


def sum_windows(a, b, first, cap):
    count, depth = a.shape
    whole = pl.BlockSpec((count, depth), lambda c, *_: (0, 0), pipeline_mode=pl.Buffered(1))
    return pl.pallas_call(
        window_kernel,
        grid_spec=pltpu.PrefetchScalarGridSpec(
            num_scalar_prefetch=1,
            grid=(first.shape[0],),
            in_specs=[whole, whole],
            out_specs=pl.BlockSpec((1, cap, depth), lambda c, *_: (c, 0, 0)),
        ),
        out_shape=jax.ShapeDtypeStruct((first.shape[0], cap, depth), jnp.float32),
        cost_estimate=pl.CostEstimate(flops=8 * a.size, bytes_accessed=12 * a.size, transcendentals=0),
        compiler_params=pltpu.CompilerParams(vmem_limit_bytes=VMEM_LIMIT),
        name="sum_windows",
    )(first, a, b)


def swap_cores(values):
    return lax.ppermute(values, "fsdp", [(0, 1), (1, 0)])


def by_core(core, mine, theirs):
    return jnp.where(core == 0, jnp.concatenate([mine, theirs]), jnp.concatenate([theirs, mine]))


def owned_rows(sorted_ids, starts, dev_cap, table_shard):
    vocab, depth = table_shard.shape
    core = lax.axis_index("fsdp")
    device = lax.axis_index("model") * sorted_ids.shape[0] + core
    padded = jnp.pad(sorted_ids, ((0, 0), (0, dev_cap)))
    first = lax.dynamic_index_in_dim(starts, device, 1, keepdims=False)
    ids = jnp.concatenate([lax.dynamic_slice(padded, (part, first[part]), (1, dev_cap))[0] for part in (1 - core, core)])
    rows = jnp.take(table_shard, jnp.clip(ids - device * vocab, 0, vocab - 1), axis=0, mode="clip")
    theirs = swap_cores(rows[:dev_cap])
    return by_core(core, rows[dev_cap:], theirs).reshape(2, dev_cap, depth)


def fast_step(sorted_ids, sorted_labels, starts, sizes, pair, halves, table_shard, gain_in, gain_out):
    model_size, fsdp_size, dev_cap, chip_cap = sizes
    vocab, depth = table_shard.shape
    chip = lax.axis_index("model")
    core = lax.axis_index("fsdp")
    device = chip * fsdp_size + core
    count = sorted_ids.shape[1]
    num_tokens = count * fsdp_size
    right = depth // 2
    left = depth - right
    own = lambda values: lax.dynamic_index_in_dim(values, core, 0, keepdims=False)
    other = lambda values: lax.dynamic_index_in_dim(values, 1 - core, 0, keepdims=False)

    my_starts = own(starts)
    blocks = lax.all_gather(pair, "model", axis=0, tiled=True)
    w_gate, w_up, w_down = (by_core(core, mine, theirs) for mine, theirs in halves)
    blocks, table_t, w_gate, w_up, w_down = lax.optimization_barrier((blocks, table_shard.T, w_gate, w_up, w_down))
    x_buf = place_rows(blocks, my_starts, count + dev_cap + 8, jnp.float32)
    normed_bf, gate_bf, up_bf, act_bf, h_res, hn_own = mlp_forward_kernel(x_buf, gain_in, gain_out, w_gate, w_up, w_down, count)
    hn_other = swap_cores(hn_own)
    lane = lax.broadcasted_iota(jnp.int32, (fsdp_size, count, LANES), 2)
    local_labels = (sorted_labels - device * vocab)[:, :, None]
    offs = jnp.where((local_labels >= 0) & (local_labels < vocab), lane - local_labels, 1)
    off_own, off_other = own(offs), other(offs)
    z_own, stat_own = head_logits(hn_own, table_t, off_own)
    z_other, stat_other = head_logits(hn_other, table_t, off_other)
    part = by_core(core, stat_own[:, :3].T, stat_other[:, :3].T)
    all_stats = lax.all_gather(part, ("model", "fsdp"), axis=0).reshape(-1, fsdp_size, 3, count)
    row_max = jnp.max(all_stats[:, :, 0], axis=0)
    sum_exp = jnp.sum(all_stats[:, :, 1] * jnp.exp(all_stats[:, :, 0] - row_max[None]), axis=0)
    label_logit = jnp.sum(all_stats[:, :, 2], axis=0)
    loss = jnp.sum(row_max + jnp.log(sum_exp) - label_logit) / num_tokens
    max_lanes = jnp.broadcast_to(row_max[:, :, None], (fsdp_size, count, LANES))
    scale_lanes = jnp.broadcast_to((1.0 / sum_exp / num_tokens)[:, :, None], (fsdp_size, count, LANES))
    inv_tokens = 1.0 / num_tokens
    dz_other, d_hn_other = head_dlogits(z_other, table_shard, other(max_lanes), other(scale_lanes), off_other, inv_tokens, left)
    d_hn_theirs = swap_cores(d_hn_other)
    dz_own, d_hn_own = head_dlogits(z_own, table_shard, own(max_lanes), own(scale_lanes), off_own, inv_tokens, left)

    first = jnp.minimum(my_starts[0:model_size * fsdp_size:fsdp_size], count - chip_cap)
    windows = sum_windows(d_hn_own, d_hn_theirs, first, chip_cap)
    windows, dz_other, dz_own = lax.optimization_barrier((windows, dz_other, dz_own))
    d_hn_left = lax.psum_scatter(windows.reshape(model_size * chip_cap, left), "model", scatter_dimension=0, tiled=True)
    d_hn_other = head_dhn(dz_other, table_shard, right, left // right)
    d_hn_theirs = swap_cores(d_hn_other)
    d_hn_own = head_dhn(dz_own, table_shard, right, left // right)
    windows = sum_windows(d_hn_own, d_hn_theirs, first, chip_cap)
    windows, dz_other, dz_own = lax.optimization_barrier((windows, dz_other, dz_own))
    d_hn_right = lax.psum_scatter(windows.reshape(model_size * chip_cap, right), "model", scatter_dimension=0, tiled=True)
    d_head = head_dtable(dz_own, hn_own, dz_other, hn_other, None)
    d_hn_left, d_hn_right, d_head = lax.optimization_barrier((d_hn_left, d_hn_right, d_head))
    d_hn = jnp.concatenate([d_hn_left, d_hn_right], axis=1)
    my_first = lax.dynamic_index_in_dim(first, chip, 0, keepdims=False)
    h_window = lax.dynamic_slice(h_res, (my_first, 0), (chip_cap, depth))
    _, norm_out_back = jax.vjp(lambda values: rms_scale(values, gain_out), h_window)
    d_hidden = norm_out_back(d_hn)[0]
    dm_blocks = lax.all_gather(d_hidden.astype(jnp.bfloat16), "model", axis=0)
    d_head = head_dtable(dz_own, hn_own, dz_other, hn_other, d_head)
    dm_blocks, d_head = lax.optimization_barrier((dm_blocks, d_head))
    d_mlp = place_rows(dm_blocks, first, count, jnp.bfloat16)

    d_gate, d_up, grad_down = mlp_dact(d_mlp, w_down, gate_bf, up_bf, act_bf)
    grad_gate = jnp.einsum("td,tf->df", normed_bf, d_gate, preferred_element_type=jnp.float32)
    grad_up = jnp.einsum("td,tf->df", normed_bf, d_up, preferred_element_type=jnp.float32)
    d_gate_own = lax.dynamic_slice(d_gate, (my_first, 0), (chip_cap, d_gate.shape[1]))
    d_up_own = lax.dynamic_slice(d_up, (my_first, 0), (chip_cap, d_up.shape[1]))
    x_window = lax.dynamic_slice(x_buf, (my_first, 0), (chip_cap, depth))
    d_normed = jnp.einsum("tf,df->td", d_gate_own, w_gate, preferred_element_type=jnp.float32) + jnp.einsum("tf,df->td", d_up_own, w_up, preferred_element_type=jnp.float32)
    _, norm_in_back = jax.vjp(lambda values: rms_scale(values, gain_in), x_window)
    d_x = d_hidden + norm_in_back(d_normed)[0]
    d_x_theirs = swap_cores(d_x)

    tile = vocab // 6
    pair_first = jnp.minimum(lax.dynamic_index_in_dim(starts, chip * fsdp_size, 1, keepdims=False), count - chip_cap)
    own_ids = jnp.stack([lax.dynamic_slice(sorted_ids, (p, pair_first[p]), (1, chip_cap))[0] for p in (core, 1 - core)]) - device * vocab
    edges = jnp.arange(vocab // tile + 1, dtype=jnp.int32) * tile
    bounds = jnp.sum((own_ids[:, :, None] < edges[None, None, :]).astype(jnp.int32), axis=1)
    grad_table = add_rows(d_head, d_x, d_x_theirs, own_ids, bounds, tile)

    grad_gate = lax.psum_scatter(grad_gate, "fsdp", scatter_dimension=0, tiled=True)
    grad_up = lax.psum_scatter(grad_up, "fsdp", scatter_dimension=0, tiled=True)
    grad_down = lax.psum_scatter(grad_down, "fsdp", scatter_dimension=0, tiled=True)
    return loss, grad_table, grad_gate, grad_up, grad_down


def capacity(tokens, shares, lists):
    mean = tokens / shares
    deviation = (mean * (1 - 1 / shares)) ** 0.5
    return -(-int((mean + 4.5 * deviation) / lists) // 16) * 16


def solution(mesh):
    fsdp_size = mesh.shape["fsdp"]
    model_size = mesh.shape["model"]
    tok_spec = P("fsdp", None)
    row_spec = P(("model", "fsdp"), None)
    weight_spec = P("fsdp", None)

    def device_step(tok_ids, tok_labels, table_shard, gate_shard, up_shard, down_shard, gain_in, gain_out):
        count = tok_ids.shape[0] * tok_ids.shape[1]
        vocab = table_shard.shape[0]
        devices = model_size * fsdp_size
        both = lax.all_gather(jnp.stack([tok_ids.reshape(-1), tok_labels.reshape(-1)]), "fsdp", axis=1, tiled=True)
        both, gate_shard, up_shard, down_shard = lax.optimization_barrier((both, gate_shard, up_shard, down_shard))
        ids, labels = lax.sort((both[0], both[1]), num_keys=1)
        sorted_ids = ids.reshape(count, fsdp_size).T
        sorted_labels = labels.reshape(count, fsdp_size).T
        edges = jnp.arange(devices + 1, dtype=jnp.int32) * vocab
        starts = jnp.sum((sorted_ids[:, :, None] < edges[None, None, :]).astype(jnp.int32), axis=1)
        dev_cap = capacity(count * fsdp_size, devices, fsdp_size)
        chip_cap = capacity(count * fsdp_size, model_size, fsdp_size)
        dev_counts = starts[:, 1:] - starts[:, :-1]
        chip_starts = starts[:, ::fsdp_size]
        chip_counts = chip_starts[:, 1:] - chip_starts[:, :-1]
        fits = (jnp.max(dev_counts) <= dev_cap) & (jnp.max(chip_counts) <= chip_cap)
        core = lax.axis_index("fsdp")
        pair = owned_rows(sorted_ids, starts, dev_cap, table_shard)
        halves = tuple((shard, swap_cores(shard)) for shard in (gate_shard, up_shard, down_shard))
        weights = (halves, table_shard, gain_in, gain_out)
        return lax.cond(
            fits,
            lambda: fast_step(sorted_ids, sorted_labels, starts, (model_size, fsdp_size, dev_cap, chip_cap), pair, *weights),
            lambda: slow_step(tok_ids, tok_labels, *weights),
        )

    return jax.shard_map(device_step, mesh=mesh, in_specs=(tok_spec, tok_spec, row_spec, weight_spec, weight_spec, weight_spec, P(), P()), out_specs=(P(), row_spec, weight_spec, weight_spec, weight_spec), check_vma=False)
```

```python
import functools

import jax
import jax.numpy as jnp
from jax import lax
from jax.experimental import pallas as pl
from jax.experimental.pallas import tpu as pltpu
from jax.sharding import PartitionSpec as P

EPS = 1e-6
VMEM_LIMIT = 63 * 1024 * 1024
LANES = 128
NN = (((1,), (0,)), ((), ()))
TN = (((0,), (0,)), ((), ()))
NT = (((1,), (1,)), ((), ()))


def rms_scale(values, gain_vec):
    mean_sq = jnp.mean(values * values, axis=-1, keepdims=True)
    return values * lax.rsqrt(mean_sq + EPS) * gain_vec


def mlp_forward(x_emb, gain_in, w_gate, w_up, w_down):
    normed_in, norm_in_back = jax.vjp(lambda values: rms_scale(values, gain_in), x_emb)
    normed_bf = normed_in.astype(jnp.bfloat16)
    gate_f = jnp.dot(normed_bf, w_gate, preferred_element_type=jnp.float32).astype(jnp.bfloat16).astype(jnp.float32)
    up_f = jnp.dot(normed_bf, w_up, preferred_element_type=jnp.float32).astype(jnp.bfloat16).astype(jnp.float32)
    gate_sig = jax.nn.sigmoid(gate_f)
    silu_gate = gate_f * gate_sig
    act_bf = (silu_gate * up_f).astype(jnp.bfloat16)
    mlp_out = jnp.dot(act_bf, w_down, preferred_element_type=jnp.float32).astype(jnp.bfloat16)
    h_res = x_emb + mlp_out.astype(jnp.float32)
    return h_res, (norm_in_back, normed_bf, gate_f, up_f, gate_sig, silu_gate, act_bf)


def mlp_backward(d_hidden, saved, w_gate, w_up, w_down):
    norm_in_back, normed_bf, gate_f, up_f, gate_sig, silu_gate, act_bf = saved
    d_mlp = d_hidden.astype(jnp.bfloat16)
    d_act = jnp.einsum("td,fd->tf", d_mlp, w_down, preferred_element_type=jnp.float32)
    grad_down = jnp.einsum("tf,td->fd", act_bf, d_mlp, preferred_element_type=jnp.float32)
    d_gate = (d_act * up_f * (gate_sig * (1.0 + gate_f * (1.0 - gate_sig)))).astype(jnp.bfloat16)
    d_up = (d_act * silu_gate).astype(jnp.bfloat16)
    grad_gate = jnp.einsum("td,tf->df", normed_bf, d_gate, preferred_element_type=jnp.float32)
    grad_up = jnp.einsum("td,tf->df", normed_bf, d_up, preferred_element_type=jnp.float32)
    d_normed = jnp.einsum("tf,df->td", d_gate, w_gate, preferred_element_type=jnp.float32) + jnp.einsum("tf,df->td", d_up, w_up, preferred_element_type=jnp.float32)
    d_x = d_hidden + norm_in_back(d_normed)[0]
    return d_x, grad_gate, grad_up, grad_down


def slow_step(tok_ids, tok_labels, halves, table_shard, gain_in, gain_out):
    fsdp_size = lax.axis_size("fsdp")
    local_count = tok_ids.shape[0] * tok_ids.shape[1]
    num_tokens = local_count * fsdp_size
    table_part = lax.all_gather(table_shard, "fsdp", axis=0, tiled=True)
    w_gate, w_up, w_down = (by_core(lax.axis_index("fsdp"), mine, theirs) for mine, theirs in halves)
    vocab_part = table_part.shape[0]
    vocab_start = lax.axis_index("model") * vocab_part
    local_ids = tok_ids.reshape(local_count) - vocab_start
    id_inside = (local_ids >= 0) & (local_ids < vocab_part)
    safe_ids = jnp.where(id_inside, local_ids, 0)
    emb_rows = jnp.where(id_inside[:, None], jnp.take(table_part, safe_ids, axis=0), 0)
    x_emb = lax.psum(emb_rows, "model").astype(jnp.float32)
    h_res, saved = mlp_forward(x_emb, gain_in, w_gate, w_up, w_down)
    hn_f, norm_out_back = jax.vjp(lambda values: rms_scale(values, gain_out), h_res)
    hn_bf = hn_f.astype(jnp.bfloat16)
    logits = jnp.einsum("td,vd->tv", hn_bf, table_part, preferred_element_type=jnp.float32)
    row_max = lax.pmax(jnp.max(logits, axis=-1), "model")
    exp_shift = jnp.exp(logits - row_max[:, None])
    local_labels = tok_labels.reshape(local_count) - vocab_start
    onehot = lax.broadcasted_iota(jnp.int32, logits.shape, 1) == local_labels[:, None]
    part_stats = jnp.stack([jnp.sum(exp_shift, axis=-1), jnp.sum(jnp.where(onehot, logits, 0.0), axis=-1)])
    tok_stats = lax.psum(part_stats, "model")
    sum_exp = tok_stats[0]
    tok_loss = row_max + jnp.log(sum_exp) - tok_stats[1]
    loss = lax.psum(jnp.sum(tok_loss), "fsdp") / num_tokens
    soft_probs = exp_shift / sum_exp[:, None]
    d_logits = (jnp.where(onehot, soft_probs - 1.0, soft_probs) / num_tokens).astype(jnp.bfloat16)
    d_head = jnp.einsum("tv,td->vd", d_logits, hn_bf, preferred_element_type=jnp.float32)
    d_hn = lax.psum(jnp.einsum("tv,vd->td", d_logits, table_part, preferred_element_type=jnp.float32), "model")
    d_hidden = norm_out_back(d_hn)[0]
    d_x, grad_gate, grad_up, grad_down = mlp_backward(d_hidden, saved, w_gate, w_up, w_down)
    d_in = jax.ops.segment_sum(jnp.where(id_inside[:, None], d_x, 0.0), safe_ids, num_segments=vocab_part)
    grad_table = lax.psum_scatter(d_head + d_in, "fsdp", scatter_dimension=0, tiled=True)
    grad_gate = lax.psum_scatter(grad_gate, "fsdp", scatter_dimension=0, tiled=True)
    grad_up = lax.psum_scatter(grad_up, "fsdp", scatter_dimension=0, tiled=True)
    grad_down = lax.psum_scatter(grad_down, "fsdp", scatter_dimension=0, tiled=True)
    return loss, grad_table, grad_gate, grad_up, grad_down


def lane_chunks(width, chunk):
    return [(lo, min(chunk, width - lo)) for lo in range(0, width, chunk)]

def logits_kernel(chunk, hn_ref, emb_ref, off_ref, z_ref, stat_ref):
    rows, vocab = z_ref.shape
    hn = hn_ref[...]
    off = off_ref[...]
    lane = lax.broadcasted_iota(jnp.int32, (rows, LANES), 1)
    run_max = jnp.full((rows, LANES), -jnp.inf, jnp.float32)
    run_sum = jnp.zeros((rows, LANES), jnp.float32)
    run_lab = jnp.zeros((rows, LANES), jnp.float32)
    for lo, width in lane_chunks(vocab, chunk):
        z = lax.dot_general(hn, emb_ref[:, lo:lo + width], NN, preferred_element_type=jnp.float32)
        z_ref[:, lo:lo + width] = z
        groups = width // LANES
        parts = [z[:, g * LANES:(g + 1) * LANES] for g in range(groups)]
        if width % LANES:
            short = width % LANES
            filler = jnp.full((rows, LANES - short), -jnp.inf, jnp.float32)
            parts.append(jnp.concatenate([z[:, groups * LANES:], filler], axis=1))
        new_max = run_max
        for g, part in enumerate(parts):
            new_max = jnp.maximum(new_max, part)
            run_lab = jnp.where(off == -(lo + g * LANES), part, run_lab)
        run_sum = run_sum * jnp.exp(run_max - new_max)
        for part in parts:
            run_sum = run_sum + jnp.exp(part - new_max)
        run_max = new_max
    row_max = jnp.max(run_max, axis=1, keepdims=True)
    row_sum = jnp.sum(run_sum * jnp.exp(run_max - row_max), axis=1, keepdims=True)
    row_lab = jnp.sum(run_lab, axis=1, keepdims=True)
    stat_ref[...] = jnp.where(lane == 0, row_max, jnp.where(lane == 1, row_sum, row_lab))


def head_logits(hn, table_t, off, blk=256, chunk=1024):
    tokens, depth = hn.shape
    vocab = table_t.shape[1]
    return pl.pallas_call(
        functools.partial(logits_kernel, chunk),
        grid=(tokens // blk,),
        in_specs=[
            pl.BlockSpec((blk, depth), lambda i: (i, 0)),
            pl.BlockSpec((depth, vocab), lambda i: (0, 0), pipeline_mode=pl.Buffered(1)),
            pl.BlockSpec((blk, LANES), lambda i: (i, 0)),
        ],
        out_specs=[
            pl.BlockSpec((blk, vocab), lambda i: (i, 0)),
            pl.BlockSpec((blk, LANES), lambda i: (i, 0)),
        ],
        out_shape=[jax.ShapeDtypeStruct((tokens, vocab), jnp.float32), jax.ShapeDtypeStruct((tokens, LANES), jnp.float32)],
        cost_estimate=pl.CostEstimate(flops=2 * tokens * vocab * depth, bytes_accessed=4 * tokens * vocab, transcendentals=tokens * vocab),
        compiler_params=pltpu.CompilerParams(vmem_limit_bytes=VMEM_LIMIT),
        name="head_logits",
    )(hn, table_t, off)


def dlogits_kernel(inv_tokens, chunk, z_ref, emb_ref, max_ref, scale_ref, off_ref, dz_ref, dhn_ref):
    vocab = z_ref.shape[1]
    row_max = max_ref[...]
    scale = scale_ref[...]
    off = off_ref[...]
    total = None
    for lo, width in lane_chunks(vocab, chunk):
        for g in range(0, width, LANES):
            lanes = min(LANES, width - g)
            cols = slice(lo + g, lo + g + lanes)
            grad = jnp.exp(z_ref[:, cols] - row_max[:, :lanes]) * scale[:, :lanes]
            grad = jnp.where(off[:, :lanes] == -(lo + g), grad - inv_tokens, grad)
            dz_ref[:, cols] = grad.astype(jnp.bfloat16)
        part = jnp.dot(dz_ref[:, lo:lo + width], emb_ref[lo:lo + width, :], preferred_element_type=jnp.float32)
        total = part if total is None else total + part
    dhn_ref[...] = total


def head_dlogits(z, table, row_max, scale, off, inv_tokens, cols, blk=512, chunk=1024):
    tokens, vocab = z.shape
    row = pl.BlockSpec((blk, LANES), lambda i: (i, 0))
    return pl.pallas_call(
        functools.partial(dlogits_kernel, inv_tokens, chunk),
        grid=(tokens // blk,),
        in_specs=[
            pl.BlockSpec((blk, vocab), lambda i: (i, 0)),
            pl.BlockSpec((vocab, cols), lambda i: (0, 0), pipeline_mode=pl.Buffered(1)),
            row,
            row,
            row,
        ],
        out_specs=[
            pl.BlockSpec((blk, vocab), lambda i: (i, 0)),
            pl.BlockSpec((blk, cols), lambda i: (i, 0)),
        ],
        out_shape=[jax.ShapeDtypeStruct((tokens, vocab), jnp.bfloat16), jax.ShapeDtypeStruct((tokens, cols), jnp.float32)],
        cost_estimate=pl.CostEstimate(flops=2 * tokens * vocab * cols, bytes_accessed=6 * tokens * vocab, transcendentals=tokens * vocab),
        compiler_params=pltpu.CompilerParams(vmem_limit_bytes=VMEM_LIMIT),
        name="head_dlogits",
    )(z, table, row_max, scale, off)


def dhn_kernel(dz_ref, emb_ref, dhn_ref):
    dhn_ref[...] = jnp.dot(dz_ref[...], emb_ref[...], preferred_element_type=jnp.float32)


def head_dhn(dz, table, cols, index, blk=512):
    tokens, vocab = dz.shape
    return pl.pallas_call(
        dhn_kernel,
        grid=(tokens // blk,),
        in_specs=[
            pl.BlockSpec((blk, vocab), lambda i: (i, 0)),
            pl.BlockSpec((vocab, cols), lambda i: (0, index), pipeline_mode=pl.Buffered(1)),
        ],
        out_specs=pl.BlockSpec((blk, cols), lambda i: (i, 0)),
        out_shape=jax.ShapeDtypeStruct((tokens, cols), jnp.float32),
        cost_estimate=pl.CostEstimate(flops=2 * tokens * vocab * cols, bytes_accessed=2 * tokens * vocab, transcendentals=0),
        compiler_params=pltpu.CompilerParams(vmem_limit_bytes=VMEM_LIMIT),
        name="head_dhn",
    )(dz, table)


def dtable_kernel(a_ref, ha_ref, b_ref, hb_ref, *refs):
    out_ref = refs[-1]
    out_ref[...] = (lax.dot_general(a_ref[...], ha_ref[...], TN, preferred_element_type=jnp.float32)
                    + lax.dot_general(b_ref[...], hb_ref[...], TN, preferred_element_type=jnp.float32))


def head_dtable(dz_a, hn_a, dz_b, hn_b, partial, tile=640, early=0.7):
    tokens, vocab = dz_a.shape
    depth = hn_a.shape[1]
    tiles = pl.cdiv(vocab, tile)
    split = int(early * tiles)
    start, steps = (0, split) if partial is None else (split, tiles - split)
    dz_spec = pl.BlockSpec((tokens, tile), lambda i: (0, i + start))
    hn_spec = pl.BlockSpec((tokens, depth), lambda i: (0, 0), pipeline_mode=pl.Buffered(1))
    rest = () if partial is None else (partial,)
    return pl.pallas_call(
        dtable_kernel,
        grid=(steps,),
        in_specs=[dz_spec, hn_spec, dz_spec, hn_spec] + [pl.BlockSpec(memory_space=pl.ANY)] * len(rest),
        out_specs=pl.BlockSpec((tile, depth), lambda i: (i + start, 0)),
        out_shape=jax.ShapeDtypeStruct((vocab, depth), jnp.float32),
        input_output_aliases={4: 0} if rest else {},
        cost_estimate=pl.CostEstimate(flops=4 * tokens * steps * tile * depth, bytes_accessed=4 * tokens * steps * tile, transcendentals=0),
        compiler_params=pltpu.CompilerParams(vmem_limit_bytes=VMEM_LIMIT),
        name="head_dtable",
    )(dz_a, hn_a, dz_b, hn_b, *rest)


def norm(values, gain):
    return values * lax.rsqrt(jnp.mean(values * values, axis=-1, keepdims=True) + EPS) * gain

def mlp_kernel(chunk, x_ref, g1_ref, g2_ref, wg_ref, wu_ref, wd_ref, a_ref, gt_ref, up_ref, q_ref, h_ref, hn_ref):
    x = x_ref[...]
    a = norm(x, g1_ref[...]).astype(jnp.bfloat16)
    a_ref[...] = a
    total = None
    for lo in range(0, gt_ref.shape[1], chunk):
        cols = slice(lo, lo + chunk)
        gt = jnp.dot(a, wg_ref[:, cols], preferred_element_type=jnp.float32).astype(jnp.bfloat16)
        up = jnp.dot(a, wu_ref[:, cols], preferred_element_type=jnp.float32).astype(jnp.bfloat16)
        gt_ref[:, cols] = gt
        up_ref[:, cols] = up
        gate = gt.astype(jnp.float32)
        q = (gate * jax.nn.sigmoid(gate) * up.astype(jnp.float32)).astype(jnp.bfloat16)
        q_ref[:, cols] = q
        part = jnp.dot(q, wd_ref[cols, :], preferred_element_type=jnp.float32)
        total = part if total is None else total + part
    h = x + total.astype(jnp.bfloat16).astype(jnp.float32)
    h_ref[...] = h
    hn_ref[...] = norm(h, g2_ref[...]).astype(jnp.bfloat16)

def mlp_forward_kernel(x, g1, g2, wg, wu, wd, tokens, blk=256, chunk=1024):
    depth = x.shape[1]
    width = wg.shape[1]
    row = lambda n: pl.BlockSpec((blk, n), lambda i: (i, 0))
    whole = lambda s: pl.BlockSpec(s, lambda i: (0, 0), pipeline_mode=pl.Buffered(1))
    shape = lambda n, t: jax.ShapeDtypeStruct((tokens, n), t)
    return pl.pallas_call(
        functools.partial(mlp_kernel, chunk),
        grid=(tokens // blk,),
        in_specs=[row(depth), whole((1, depth)), whole((1, depth)), whole(wg.shape), whole(wu.shape), whole(wd.shape)],
        out_specs=[row(depth), row(width), row(width), row(width), row(depth), row(depth)],
        out_shape=[shape(depth, jnp.bfloat16), shape(width, jnp.bfloat16), shape(width, jnp.bfloat16), shape(width, jnp.bfloat16), shape(depth, jnp.float32), shape(depth, jnp.bfloat16)],
        cost_estimate=pl.CostEstimate(flops=6 * tokens * width * depth, bytes_accessed=6 * tokens * width, transcendentals=tokens * width),
        compiler_params=pltpu.CompilerParams(vmem_limit_bytes=VMEM_LIMIT),
        name="mlp_forward",
    )(x, g1.reshape(1, -1), g2.reshape(1, -1), wg, wu, wd)

def dact_kernel(rows, dm_ref, wd_ref, gt_ref, up_ref, q_ref, dgt_ref, dup_ref, dwd_ref):
    for lo in range(0, dm_ref.shape[0], rows):
        part = slice(lo, lo + rows)
        dq = lax.dot_general(dm_ref[part, :], wd_ref[...], NT, preferred_element_type=jnp.float32)
        gate = gt_ref[part, :].astype(jnp.float32)
        up = up_ref[part, :].astype(jnp.float32)
        sig = jax.nn.sigmoid(gate)
        dgt_ref[part, :] = (dq * up * (sig * (1.0 + gate * (1.0 - sig)))).astype(jnp.bfloat16)
        dup_ref[part, :] = (dq * (gate * sig)).astype(jnp.bfloat16)
    dwd_ref[...] = lax.dot_general(q_ref[...], dm_ref[...], TN, preferred_element_type=jnp.float32)


def mlp_dact(dm, wd, gt, up, q, cols=512, rows=512):
    tokens, depth = dm.shape
    width = wd.shape[0]
    col = pl.BlockSpec((tokens, cols), lambda j: (0, j))
    row = pl.BlockSpec((cols, depth), lambda j: (j, 0))
    return pl.pallas_call(
        functools.partial(dact_kernel, rows),
        grid=(width // cols,),
        in_specs=[pl.BlockSpec((tokens, depth), lambda j: (0, 0), pipeline_mode=pl.Buffered(1)), row, col, col, col],
        out_specs=[col, col, row],
        out_shape=[jax.ShapeDtypeStruct((tokens, width), jnp.bfloat16)] * 2 + [jax.ShapeDtypeStruct((width, depth), jnp.float32)],
        cost_estimate=pl.CostEstimate(flops=4 * tokens * width * depth, bytes_accessed=10 * tokens * width, transcendentals=tokens * width),
        compiler_params=pltpu.CompilerParams(vmem_limit_bytes=VMEM_LIMIT),
        name="mlp_dact",
    )(dm, wd, gt, up, q)


def add_rows_kernel(bound_ref, ids_ref, base_ref, own_ref, theirs_ref, out_ref):
    tile = pl.program_id(0)
    out_ref[...] = base_ref[...]
    start = tile * out_ref.shape[0]
    for part, rows_ref in enumerate((own_ref, theirs_ref)):
        def body(t, carry, part=part, rows_ref=rows_ref):
            row = ids_ref[part, t] - start
            out_ref[pl.ds(row, 1), :] = out_ref[pl.ds(row, 1), :] + rows_ref[pl.ds(t, 1), :]
            return carry
        lax.fori_loop(bound_ref[part, tile], bound_ref[part, tile + 1], body, 0)


def add_rows(base, own, theirs, ids, bounds, tile):
    vocab, depth = base.shape
    whole = pl.BlockSpec(own.shape, lambda i, *_: (0, 0), pipeline_mode=pl.Buffered(1))
    return pl.pallas_call(
        add_rows_kernel,
        grid_spec=pltpu.PrefetchScalarGridSpec(
            num_scalar_prefetch=2,
            grid=(vocab // tile,),
            in_specs=[pl.BlockSpec((tile, depth), lambda i, *_: (i, 0)), whole, whole],
            out_specs=pl.BlockSpec((tile, depth), lambda i, *_: (i, 0)),
        ),
        out_shape=jax.ShapeDtypeStruct(base.shape, base.dtype),
        input_output_aliases={2: 0},
        cost_estimate=pl.CostEstimate(flops=2 * vocab * depth, bytes_accessed=8 * vocab * depth, transcendentals=0),
        compiler_params=pltpu.CompilerParams(vmem_limit_bytes=VMEM_LIMIT),
        name="add_rows",
    )(bounds, ids, base, own, theirs)


def place_kernel(start_ref, block_ref, out_ref, *scratch):
    rows = scratch[0] if scratch else out_ref
    _, cap, depth = block_ref.shape
    start = start_ref[pl.program_id(0)]
    sub = lax.broadcasted_iota(jnp.int32, (8, depth), 0)
    base = pl.multiple_of(start // 8 * 8, 8)
    shift = start % 8
    before = rows[pl.ds(base, 8), :]
    for j in range(0, cap, 16):
        piece = block_ref[0, j:j + 16, :].astype(jnp.float32)
        for k in (0, 8):
            turned = pltpu.roll(piece[k:k + 8], shift, 0)
            rows[pl.ds(pl.multiple_of(base + (j + k), 8), 8), :] = jnp.where(sub < shift, before, turned)
            before = turned
    tail = pl.ds(pl.multiple_of(base + cap, 8), 8)
    rows[tail, :] = jnp.where(sub < shift, before, rows[tail, :])
    if scratch:
        @pl.when(pl.program_id(0) == pl.num_programs(0) - 1)
        def _():
            out_ref[...] = rows[:out_ref.shape[0]].astype(out_ref.dtype)


def place_rows(blocks, starts, count, dtype):
    number, cap, depth = blocks.shape
    return pl.pallas_call(
        place_kernel,
        grid_spec=pltpu.PrefetchScalarGridSpec(
            num_scalar_prefetch=1,
            grid=(number,),
            in_specs=[pl.BlockSpec((1, cap, depth), lambda b, *_: (b, 0, 0))],
            out_specs=pl.BlockSpec((count, depth), lambda b, *_: (0, 0)),
            scratch_shapes=[] if dtype == jnp.float32 else [pltpu.VMEM((count + 8, depth), jnp.float32)],
        ),
        out_shape=jax.ShapeDtypeStruct((count, depth), dtype),
        cost_estimate=pl.CostEstimate(flops=8 * count * depth, bytes_accessed=8 * count * depth, transcendentals=0),
        compiler_params=pltpu.CompilerParams(vmem_limit_bytes=VMEM_LIMIT),
        name="place_rows",
    )(starts, blocks)


def window_kernel(first_ref, a_ref, b_ref, out_ref):
    count, _ = a_ref.shape
    cap = out_ref.shape[1]
    first = first_ref[pl.program_id(0)]
    base = pl.multiple_of(jnp.minimum(first // 8, (count - cap) // 8 - 1) * 8, 8)
    keep = 8 - (first - base)
    sub = lax.broadcasted_iota(jnp.int32, (8, a_ref.shape[1]), 0)
    here = None
    for j in range(0, cap + 8, 8):
        rows = pl.ds(pl.multiple_of(base + j, 8), 8)
        turned = pltpu.roll(a_ref[rows, :] + b_ref[rows, :], keep % 8, 0)
        if j:
            out_ref[0, j - 8:j, :] = jnp.where(sub < keep, here, turned)
        here = turned


def sum_windows(a, b, first, cap):
    count, depth = a.shape
    whole = pl.BlockSpec((count, depth), lambda c, *_: (0, 0), pipeline_mode=pl.Buffered(1))
    return pl.pallas_call(
        window_kernel,
        grid_spec=pltpu.PrefetchScalarGridSpec(
            num_scalar_prefetch=1,
            grid=(first.shape[0],),
            in_specs=[whole, whole],
            out_specs=pl.BlockSpec((1, cap, depth), lambda c, *_: (c, 0, 0)),
        ),
        out_shape=jax.ShapeDtypeStruct((first.shape[0], cap, depth), jnp.float32),
        cost_estimate=pl.CostEstimate(flops=8 * a.size, bytes_accessed=12 * a.size, transcendentals=0),
        compiler_params=pltpu.CompilerParams(vmem_limit_bytes=VMEM_LIMIT),
        name="sum_windows",
    )(first, a, b)


def swap_cores(values):
    return lax.ppermute(values, "fsdp", [(0, 1), (1, 0)])


def by_core(core, mine, theirs):
    return jnp.where(core == 0, jnp.concatenate([mine, theirs]), jnp.concatenate([theirs, mine]))


def owned_rows(sorted_ids, starts, dev_cap, table_shard):
    vocab, depth = table_shard.shape
    core = lax.axis_index("fsdp")
    device = lax.axis_index("model") * sorted_ids.shape[0] + core
    padded = jnp.pad(sorted_ids, ((0, 0), (0, dev_cap)))
    first = lax.dynamic_index_in_dim(starts, device, 1, keepdims=False)
    ids = jnp.concatenate([lax.dynamic_slice(padded, (part, first[part]), (1, dev_cap))[0] for part in (1 - core, core)])
    rows = jnp.take(table_shard, jnp.clip(ids - device * vocab, 0, vocab - 1), axis=0, mode="clip")
    theirs = swap_cores(rows[:dev_cap])
    return by_core(core, rows[dev_cap:], theirs).reshape(2, dev_cap, depth)


def fast_step(sorted_ids, sorted_labels, starts, sizes, pair, halves, table_shard, gain_in, gain_out):
    model_size, fsdp_size, dev_cap, chip_cap = sizes
    vocab, depth = table_shard.shape
    chip = lax.axis_index("model")
    core = lax.axis_index("fsdp")
    device = chip * fsdp_size + core
    count = sorted_ids.shape[1]
    num_tokens = count * fsdp_size
    right = depth // 2
    left = depth - right
    own = lambda values: lax.dynamic_index_in_dim(values, core, 0, keepdims=False)
    other = lambda values: lax.dynamic_index_in_dim(values, 1 - core, 0, keepdims=False)

    my_starts = own(starts)
    blocks = lax.all_gather(pair, "model", axis=0, tiled=True)
    w_gate, w_up, w_down = (by_core(core, mine, theirs) for mine, theirs in halves)
    blocks, table_t, w_gate, w_up, w_down = lax.optimization_barrier((blocks, table_shard.T, w_gate, w_up, w_down))
    x_buf = place_rows(blocks, my_starts, count + dev_cap + 8, jnp.float32)
    normed_bf, gate_bf, up_bf, act_bf, h_res, hn_own = mlp_forward_kernel(x_buf, gain_in, gain_out, w_gate, w_up, w_down, count)
    hn_other = swap_cores(hn_own)
    lane = lax.broadcasted_iota(jnp.int32, (fsdp_size, count, LANES), 2)
    local_labels = (sorted_labels - device * vocab)[:, :, None]
    offs = jnp.where((local_labels >= 0) & (local_labels < vocab), lane - local_labels, 1)
    off_own, off_other = own(offs), other(offs)
    z_own, stat_own = head_logits(hn_own, table_t, off_own)
    z_other, stat_other = head_logits(hn_other, table_t, off_other)
    part = by_core(core, stat_own[:, :3].T, stat_other[:, :3].T)
    all_stats = lax.all_gather(part, ("model", "fsdp"), axis=0).reshape(-1, fsdp_size, 3, count)
    row_max = jnp.max(all_stats[:, :, 0], axis=0)
    sum_exp = jnp.sum(all_stats[:, :, 1] * jnp.exp(all_stats[:, :, 0] - row_max[None]), axis=0)
    label_logit = jnp.sum(all_stats[:, :, 2], axis=0)
    loss = jnp.sum(row_max + jnp.log(sum_exp) - label_logit) / num_tokens
    max_lanes = jnp.broadcast_to(row_max[:, :, None], (fsdp_size, count, LANES))
    scale_lanes = jnp.broadcast_to((1.0 / sum_exp / num_tokens)[:, :, None], (fsdp_size, count, LANES))
    inv_tokens = 1.0 / num_tokens
    dz_other, d_hn_other = head_dlogits(z_other, table_shard, other(max_lanes), other(scale_lanes), off_other, inv_tokens, left)
    d_hn_theirs = swap_cores(d_hn_other)
    dz_own, d_hn_own = head_dlogits(z_own, table_shard, own(max_lanes), own(scale_lanes), off_own, inv_tokens, left)

    first = jnp.minimum(my_starts[0:model_size * fsdp_size:fsdp_size], count - chip_cap)
    windows = sum_windows(d_hn_own, d_hn_theirs, first, chip_cap)
    windows, dz_other, dz_own = lax.optimization_barrier((windows, dz_other, dz_own))
    d_hn_left = lax.psum_scatter(windows.reshape(model_size * chip_cap, left), "model", scatter_dimension=0, tiled=True)
    d_hn_other = head_dhn(dz_other, table_shard, right, left // right)
    d_hn_theirs = swap_cores(d_hn_other)
    d_hn_own = head_dhn(dz_own, table_shard, right, left // right)
    windows = sum_windows(d_hn_own, d_hn_theirs, first, chip_cap)
    windows, dz_other, dz_own = lax.optimization_barrier((windows, dz_other, dz_own))
    d_hn_right = lax.psum_scatter(windows.reshape(model_size * chip_cap, right), "model", scatter_dimension=0, tiled=True)
    d_head = head_dtable(dz_own, hn_own, dz_other, hn_other, None)
    d_hn_left, d_hn_right, d_head = lax.optimization_barrier((d_hn_left, d_hn_right, d_head))
    d_hn = jnp.concatenate([d_hn_left, d_hn_right], axis=1)
    my_first = lax.dynamic_index_in_dim(first, chip, 0, keepdims=False)
    h_window = lax.dynamic_slice(h_res, (my_first, 0), (chip_cap, depth))
    _, norm_out_back = jax.vjp(lambda values: rms_scale(values, gain_out), h_window)
    d_hidden = norm_out_back(d_hn)[0]
    dm_blocks = lax.all_gather(d_hidden.astype(jnp.bfloat16), "model", axis=0)
    d_head = head_dtable(dz_own, hn_own, dz_other, hn_other, d_head)
    dm_blocks, d_head = lax.optimization_barrier((dm_blocks, d_head))
    d_mlp = place_rows(dm_blocks, first, count, jnp.bfloat16)

    d_gate, d_up, grad_down = mlp_dact(d_mlp, w_down, gate_bf, up_bf, act_bf)
    d_gate_own = lax.dynamic_slice(d_gate, (my_first, 0), (chip_cap, d_gate.shape[1]))
    d_up_own = lax.dynamic_slice(d_up, (my_first, 0), (chip_cap, d_up.shape[1]))
    x_window = lax.dynamic_slice(x_buf, (my_first, 0), (chip_cap, depth))
    d_normed = jnp.einsum("tf,df->td", d_gate_own, w_gate, preferred_element_type=jnp.float32) + jnp.einsum("tf,df->td", d_up_own, w_up, preferred_element_type=jnp.float32)
    _, norm_in_back = jax.vjp(lambda values: rms_scale(values, gain_in), x_window)
    d_x = d_hidden + norm_in_back(d_normed)[0]
    d_x_theirs = swap_cores(d_x)

    tile = vocab // 6
    pair_first = jnp.minimum(lax.dynamic_index_in_dim(starts, chip * fsdp_size, 1, keepdims=False), count - chip_cap)
    own_ids = jnp.stack([lax.dynamic_slice(sorted_ids, (p, pair_first[p]), (1, chip_cap))[0] for p in (core, 1 - core)]) - device * vocab
    edges = jnp.arange(vocab // tile + 1, dtype=jnp.int32) * tile
    bounds = jnp.sum((own_ids[:, :, None] < edges[None, None, :]).astype(jnp.int32), axis=1)
    d_gate, d_up, d_x, own_ids, bounds = lax.optimization_barrier((d_gate, d_up, d_x, own_ids, bounds))
    grad_gate = jnp.einsum("td,tf->df", normed_bf, d_gate, preferred_element_type=jnp.float32)
    grad_up = jnp.einsum("td,tf->df", normed_bf, d_up, preferred_element_type=jnp.float32)
    grad_table = add_rows(d_head, d_x, d_x_theirs, own_ids, bounds, tile)

    grad_gate = lax.psum_scatter(grad_gate, "fsdp", scatter_dimension=0, tiled=True)
    grad_up = lax.psum_scatter(grad_up, "fsdp", scatter_dimension=0, tiled=True)
    grad_down = lax.psum_scatter(grad_down, "fsdp", scatter_dimension=0, tiled=True)
    return loss, grad_table, grad_gate, grad_up, grad_down


def capacity(tokens, shares, lists):
    mean = tokens / shares
    deviation = (mean * (1 - 1 / shares)) ** 0.5
    return -(-int((mean + 4.5 * deviation) / lists) // 16) * 16


def solution(mesh):
    fsdp_size = mesh.shape["fsdp"]
    model_size = mesh.shape["model"]
    tok_spec = P("fsdp", None)
    row_spec = P(("model", "fsdp"), None)
    weight_spec = P("fsdp", None)

    def device_step(tok_ids, tok_labels, table_shard, gate_shard, up_shard, down_shard, gain_in, gain_out):
        count = tok_ids.shape[0] * tok_ids.shape[1]
        vocab = table_shard.shape[0]
        devices = model_size * fsdp_size
        both = lax.all_gather(jnp.stack([tok_ids.reshape(-1), tok_labels.reshape(-1)]), "fsdp", axis=1, tiled=True)
        both, gate_shard, up_shard, down_shard = lax.optimization_barrier((both, gate_shard, up_shard, down_shard))
        ids, labels = lax.sort((both[0], both[1]), num_keys=1)
        sorted_ids = ids.reshape(count, fsdp_size).T
        sorted_labels = labels.reshape(count, fsdp_size).T
        edges = jnp.arange(devices + 1, dtype=jnp.int32) * vocab
        starts = jnp.sum((sorted_ids[:, :, None] < edges[None, None, :]).astype(jnp.int32), axis=1)
        dev_cap = capacity(count * fsdp_size, devices, fsdp_size)
        chip_cap = capacity(count * fsdp_size, model_size, fsdp_size)
        dev_counts = starts[:, 1:] - starts[:, :-1]
        chip_starts = starts[:, ::fsdp_size]
        chip_counts = chip_starts[:, 1:] - chip_starts[:, :-1]
        fits = (jnp.max(dev_counts) <= dev_cap) & (jnp.max(chip_counts) <= chip_cap)
        core = lax.axis_index("fsdp")
        pair = owned_rows(sorted_ids, starts, dev_cap, table_shard)
        halves = tuple((shard, swap_cores(shard)) for shard in (gate_shard, up_shard, down_shard))
        weights = (halves, table_shard, gain_in, gain_out)
        return lax.cond(
            fits,
            lambda: fast_step(sorted_ids, sorted_labels, starts, (model_size, fsdp_size, dev_cap, chip_cap), pair, *weights),
            lambda: slow_step(tok_ids, tok_labels, *weights),
        )

    return jax.shard_map(device_step, mesh=mesh, in_specs=(tok_spec, tok_spec, row_spec, weight_spec, weight_spec, weight_spec, P(), P()), out_specs=(P(), row_spec, weight_spec, weight_spec, weight_spec), check_vma=False)
```
